8 devices in a mesh: case: 1 (over z), model: 2 (over y), ens: 4 (over x, core).
Axes of the slice: x: 2, y: 2, z: 1, core: 2. Of those that a mesh axis runs over, the one named last changes fastest.
Arguments:
- ens_init: float32 [16, 5120, 64], P(('case', 'ens'), None, 'model')
- mix_op: bfloat16 [5120, 5120], replicated
- w_in: bfloat16 [3, 64, 1024], P(None, None, 'model')
- w_out: bfloat16 [3, 1024, 64], P(None, 'model')
- obs_val: float32 [2, 5120, 32], P(None, ('case', 'ens', 'model'))
- obs_prec: float32 [5120, 32], P(('case', 'ens', 'model'))
- obs_idx: int32 [32], replicated
- inflation: float32 [1], replicated
Outputs:
- output: float32 [16, 5120, 64], P(('case', 'ens'), None, 'model')
All inputs are finite; a program needn't handle non-finite values.
Results may differ from the reference program's by a relative error of at most 0.0151655.
Values are sent between devices in bfloat16 or wider.
A program may use at most 1 GiB of HBM per device.

```python
import jax
import jax.numpy as jnp
from jax import lax

COLS = 5120
VARS = 64
HIDDEN = 1024
OBS_VARS = 32
LAYERS = 3
CYCLES = 2
MEMBERS = 16
NS_STEPS = 12
COL_BLOCK = 640


def setup_inputs(seed: int = 0, part: int = 0) -> dict:
    shared_keys = jax.random.split(jax.random.key(seed), 5)
    part_keys = jax.random.split(jax.random.fold_in(jax.random.key(seed + 1), part), 4)
    base_state = jax.random.normal(part_keys[0], (COLS, VARS), jnp.float32)
    spread = jax.random.normal(part_keys[1], (MEMBERS, COLS, VARS), jnp.float32)
    ens_init = base_state[None] + 0.4 * spread
    obs_val = jax.random.normal(part_keys[2], (CYCLES, COLS, OBS_VARS), jnp.float32)
    obs_prec = jax.random.uniform(part_keys[3], (COLS, OBS_VARS), jnp.float32, 0.75, 5.25)
    mix_op = (jax.random.normal(shared_keys[0], (COLS, COLS), jnp.float32) * COLS ** -0.5).astype(jnp.bfloat16)
    w_in = (jax.random.normal(shared_keys[1], (LAYERS, VARS, HIDDEN), jnp.float32) * VARS ** -0.5).astype(jnp.bfloat16)
    w_out = (jax.random.normal(shared_keys[2], (LAYERS, HIDDEN, VARS), jnp.float32) * (0.5 * HIDDEN ** -0.5)).astype(jnp.bfloat16)
    obs_idx = jax.random.permutation(shared_keys[3], VARS)[:OBS_VARS].astype(jnp.int32)
    inflation = jax.random.uniform(shared_keys[4], (1,), jnp.float32, 1.0, 1.6)
    return dict(ens_init=ens_init, mix_op=mix_op, w_in=w_in, w_out=w_out, obs_val=obs_val, obs_prec=obs_prec, obs_idx=obs_idx, inflation=inflation)


def forecast_member(member, mix_op, w_in, w_out):
    def layer_step(state_now, weights):
        w_first, w_second = weights
        mix_out = jnp.dot(mix_op, state_now.astype(jnp.bfloat16), preferred_element_type=jnp.float32).astype(jnp.bfloat16)
        hidden = jax.nn.gelu(jnp.dot(mix_out, w_first, preferred_element_type=jnp.float32), approximate=True)
        update = jnp.dot(hidden.astype(jnp.bfloat16), w_second, preferred_element_type=jnp.float32)
        return state_now + update, None
    result, unused = lax.scan(layer_step, member, (w_in, w_out))
    return result


def analyse_block(col_block, obs_now, prec_now, obs_idx, inflation):
    ens_mean = jnp.mean(col_block, axis=1)
    anomaly = col_block - ens_mean[:, None, :]
    obs_anom = jnp.take(anomaly, obs_idx, axis=2)
    innovation = obs_now - jnp.take(ens_mean, obs_idx, axis=1)
    weighted = obs_anom * prec_now[:, None, :]
    identity = jnp.eye(MEMBERS, dtype=jnp.float32)
    a_tilde = ((MEMBERS - 1) / inflation[0]) * identity + jnp.einsum('bip,bjp->bij', weighted, obs_anom)
    trace_sum = jnp.trace(a_tilde, axis1=1, axis2=2)[:, None, None]
    b_mat = a_tilde / trace_sum
    z_mat = jnp.broadcast_to(identity, a_tilde.shape)
    for ns_step in range(NS_STEPS):
        t_mat = 1.5 * identity - 0.5 * jnp.einsum('bij,bjk->bik', z_mat, b_mat)
        b_mat = jnp.einsum('bij,bjk->bik', b_mat, t_mat)
        z_mat = jnp.einsum('bij,bjk->bik', t_mat, z_mat)
    sqrt_inv = z_mat / jnp.sqrt(trace_sum)
    gain_vec = jnp.einsum('bip,bp->bi', weighted, innovation)
    half_step = jnp.einsum('bij,bj->bi', sqrt_inv, gain_vec)
    w_mean = jnp.einsum('bij,bj->bi', sqrt_inv, half_step)
    w_full = (MEMBERS - 1) ** 0.5 * sqrt_inv + w_mean[:, :, None]
    return ens_mean[:, None, :] + jnp.einsum('bik,biv->bkv', w_full, anomaly)


def reference(ens_init, mix_op, w_in, w_out, obs_val, obs_prec, obs_idx, inflation):
    n_blocks = COLS // COL_BLOCK
    prec_blocks = obs_prec.reshape(n_blocks, COL_BLOCK, OBS_VARS)

    def forecast_one(member):
        return forecast_member(member, mix_op, w_in, w_out)

    def analyse_pieces(pieces):
        return analyse_block(pieces[0], pieces[1], pieces[2], obs_idx, inflation)

    def run_cycle(ens_state, obs_now):
        ens_state = lax.map(forecast_one, ens_state)
        col_blocks = ens_state.reshape(MEMBERS, n_blocks, COL_BLOCK, VARS).transpose(1, 2, 0, 3)
        obs_blocks = obs_now.reshape(n_blocks, COL_BLOCK, OBS_VARS)
        analysed = lax.map(analyse_pieces, (col_blocks, obs_blocks, prec_blocks))
        return analysed.transpose(2, 0, 1, 3).reshape(MEMBERS, COLS, VARS), None

    final_state, unused = lax.scan(run_cycle, ens_init, obs_val)
    return final_state
```

```python
import functools
import math

import jax
import jax.numpy as jnp
from jax import lax
from jax.experimental import pallas as pl
from jax.experimental.pallas import tpu as pltpu
from jax.sharding import PartitionSpec as P

MESH = pl.DeviceIdType.MESH
K = 16
COLS = 5120
VARS = 64
HID = 1024
BLK = 640
LANE = 128
TILES = 5
ROWS = 512
HALF = 2560
NS_STEPS = 12
VMEM_LIMIT = 64 * 1024 * 1024 - 64 * 1024
F32 = jnp.float32
BF16 = jnp.bfloat16
C0 = math.sqrt(2.0 / math.pi)
C1 = 2.0 * C0
C2 = 8.0 * 0.044715 * C0


def coords():
    e = lax.axis_index("ens")
    return e // 2, lax.axis_index("model"), e % 2


def dev(x, y, c):
    return {"model": y, "ens": 2 * x + c}


def greet():
    x, y, c = coords()
    barrier = pltpu.get_barrier_semaphore()
    for r in range(1, 8):
        dx, dy, dc = r // 4, (r // 2) % 2, r % 2
        pl.semaphore_signal(barrier, inc=1, device_id=dev((x + dx) % 2, (y + dy) % 2, (c + dc) % 2), device_id_type=MESH)
    pl.semaphore_wait(barrier, 7)


def await_bytes(ref, sem):
    pltpu.make_async_copy(ref, ref, sem).wait()


def gather_kernel(ens_ref, w_ref, u_ref, out_ref, wall_ref, uall_ref, send, recv, wsend, wrecv, wloc):
    x, y, c = coords()
    greet()
    v0 = pl.multiple_of(32 * y, 32)

    def piece(h):
        return ens_ref.at[:, :, pl.ds(HALF * h, HALF)], out_ref.at[:, pl.ds(v0, 32), :]

    for h in range(2):
        src, dst = piece(h)
        own = jnp.logical_and(c == y, c == h)

        @pl.when(jnp.logical_not(own))
        def _():
            pltpu.make_async_remote_copy(src, dst, send.at[h], recv.at[y], device_id=dev(x, c, h), device_id_type=MESH).start()

        @pl.when(own)
        def _():
            pltpu.make_async_copy(src, dst, recv.at[y]).start()

    weights = ((w_ref, wall_ref), (u_ref, uall_ref))
    for n, (src, dst) in enumerate(weights):
        pltpu.make_async_remote_copy(src, dst.at[y], wsend.at[n], wrecv.at[n], device_id=dev(x, 1 - y, c), device_id_type=MESH).start()
        pltpu.make_async_copy(src, dst.at[y], wloc.at[n]).start()
    for n, (src, dst) in enumerate(weights):
        pltpu.make_async_copy(src, dst.at[y], wloc.at[n]).wait()
        pltpu.make_async_remote_copy(src, dst.at[1 - y], wsend.at[n], wrecv.at[n], device_id=dev(x, 1 - y, c), device_id_type=MESH).wait()
    for h in range(2):
        src, dst = piece(h)
        own = jnp.logical_and(c == y, c == h)

        @pl.when(jnp.logical_not(own))
        def _():
            pltpu.make_async_remote_copy(src, dst, send.at[h], recv.at[y], device_id=dev(x, c, h), device_id_type=MESH).wait_send()
    for s in range(2):
        await_bytes(out_ref.at[:, pl.ds(32 * s, 32), :], recv.at[s])


def gather_state(ens_t, w_in, w_out_t):
    vm = pl.BlockSpec(memory_space=pltpu.VMEM)
    hbm = pl.BlockSpec(memory_space=pl.ANY)
    dma = pltpu.SemaphoreType.DMA
    return pl.pallas_call(
        gather_kernel,
        out_shape=(
            jax.ShapeDtypeStruct((4, VARS, HALF), F32),
            jax.ShapeDtypeStruct((2,) + w_in.shape, BF16),
            jax.ShapeDtypeStruct((2,) + w_out_t.shape, BF16),
        ),
        in_specs=[vm, vm, vm],
        out_specs=(hbm, hbm, hbm),
        scratch_shapes=[dma((2,)), dma((2,)), dma((2,)), dma((2,)), dma((2,))],
        compiler_params=pltpu.CompilerParams(collective_id=1, has_side_effects=True, vmem_limit_bytes=16 * 1024 * 1024),
        name="gather_state",
    )(ens_t, w_in, w_out_t)


def forecast_kernel(layers, ht_ref, a_ref, w_ref, u_ref, out_ref, a_vm, hb, hf, mt, st, a_sem, xsend, xrecv, send, recv):
    x, y, c = coords()
    partner = dev(x, y, 1 - c)
    greet()

    def a_copy(t, q):
        row = pl.multiple_of((4 * c + q) * BLK + LANE * t, LANE)
        return pltpu.make_async_copy(a_ref.at[pl.ds(row, LANE), :], a_vm.at[t, pl.ds(LANE * q, LANE), :], a_sem.at[t, q])

    for t in range(TILES):
        for q in range(4):
            a_copy(t, q).start()

    def share(buf, t):
        lane = pl.multiple_of(LANE * t, LANE)
        piece = hb.at[buf, pl.ds(4 * c, 4), pl.ds(lane, LANE), :]
        return pltpu.make_async_remote_copy(piece, piece, xsend.at[buf, t], xrecv.at[buf, t], device_id=partner, device_id_type=MESH)

    for t in range(TILES):
        for q in range(4):
            part = ht_ref[:, BLK * q + LANE * t:BLK * q + LANE * (t + 1)].T
            hf[t, LANE * q:LANE * (q + 1), :] = part
            hb[0, 4 * c + q, LANE * t:LANE * (t + 1), :] = part.astype(BF16)
        share(0, t).start()

    def await_share(buf, t):
        lane = pl.multiple_of(LANE * t, LANE)
        await_bytes(hb.at[buf, pl.ds(4 * (1 - c), 4), pl.ds(lane, LANE), :], xrecv.at[buf, t])

    own_half = x == c
    mine = 4 * (2 * x + y)

    def ship(t, q):
        c2, y2 = q // 2, q % 2
        lane = pl.multiple_of(LANE * t, LANE)
        src = st.at[t, :, :, pl.ds(LANE * q, LANE)]
        dst = out_ref.at[pl.ds(mine, 4), :, pl.ds(lane, LANE)]
        is_self = jnp.logical_and(own_half, jnp.logical_and(c == c2, y == y2))
        rsem = recv.at[t, 2 * x + y]
        def local():
            return pltpu.make_async_copy(src, dst, rsem)

        def remote():
            return pltpu.make_async_remote_copy(src, dst, send.at[t, q], rsem, device_id=dev(c, y2, c2), device_id_type=MESH)
        return is_self, local, remote

    def layer_body(layer, carry):
        cur = lax.rem(layer, 2)
        nxt = 1 - cur
        for t in range(TILES):
            await_share(cur, t)
            share(cur, t).wait_send()

        def tile_body(t, carry2):
            @pl.when(layer == 0)
            def _():
                for q in range(4):
                    a_copy(t, q).wait()
            state = hb[cur].reshape(COLS, 4 * VARS)
            mixed = jnp.dot(a_vm[t], state, preferred_element_type=F32)
            mt[...] = mixed.astype(BF16)
            for p in range(2):
                lhs = mt[:, 128 * p:128 * (p + 1)]
                total = None
                for n in range(8):
                    h = jnp.dot(lhs, w_ref[layer, :, 256 * n:256 * (n + 1)], preferred_element_type=F32)
                    z = h * (C1 + C2 * (h * h))
                    q_act = (h + h * jnp.tanh(z)).astype(BF16)
                    part = jnp.dot(q_act, u_ref[layer, 256 * n:256 * (n + 1), :], preferred_element_type=F32)
                    total = part if total is None else total + part
                hf[t, :, 128 * p:128 * (p + 1)] = hf[t, :, 128 * p:128 * (p + 1)] + total

            @pl.when(layer < layers - 1)
            def _():
                lane = pl.multiple_of(LANE * t, LANE)
                for q in range(4):
                    hb[nxt, 4 * c + q, pl.ds(lane, LANE), :] = hf[t, LANE * q:LANE * (q + 1), :].astype(BF16)
                share(nxt, t).start()

            @pl.when(layer == layers - 1)
            def _():
                for q in range(4):
                    st[t, :, :, LANE * q:LANE * (q + 1)] = hf[t, LANE * q:LANE * (q + 1), :].T.reshape(4, VARS, LANE)
                for q in range(4):
                    is_self, local, remote = ship(t, q)

                    @pl.when(is_self)
                    def _():
                        local().start()

                    @pl.when(jnp.logical_not(is_self))
                    def _():
                        remote().start()
            return carry2

        return lax.fori_loop(0, TILES, tile_body, carry)

    lax.fori_loop(0, layers, layer_body, 0)

    for t in range(TILES):
        for q in range(4):
            is_self, local, remote = ship(t, q)

            @pl.when(jnp.logical_not(is_self))
            def _():
                remote().wait_send()
    for t in range(TILES):
        for s in range(4):
            await_bytes(out_ref.at[4 * s:4 * s + 4, :, LANE * t:LANE * (t + 1)], recv.at[t, s])


def forecast(ht, mix_op, w_pair, u_pair):
    vm = pl.BlockSpec(memory_space=pltpu.VMEM)
    hbm = pl.BlockSpec(memory_space=pl.ANY)
    dma = pltpu.SemaphoreType.DMA
    layers = w_pair.shape[0]
    return pl.pallas_call(
        functools.partial(forecast_kernel, layers),
        out_shape=jax.ShapeDtypeStruct((K, VARS, BLK), F32),
        in_specs=[vm, hbm, vm, vm],
        out_specs=hbm,
        scratch_shapes=[
            pltpu.VMEM((TILES, ROWS, COLS), BF16),
            pltpu.VMEM((2, 8, BLK, 4 * VARS), BF16),
            pltpu.VMEM((TILES, ROWS, 4 * VARS), F32),
            pltpu.VMEM((ROWS, 4 * VARS), BF16),
            pltpu.VMEM((TILES, 4, VARS, ROWS), F32),
            dma((TILES, 4)),
            dma((2, TILES)),
            dma((2, TILES)),
            dma((TILES, 4)),
            dma((TILES, 4)),
        ],
        compiler_params=pltpu.CompilerParams(collective_id=2, has_side_effects=True, vmem_limit_bytes=VMEM_LIMIT),
        name="forecast",
    )(ht, mix_op, w_pair, u_pair)


def bcast(ref, row):
    return ref[pl.ds(row, 8, stride=0), :]


def right_factor(ref):
    top = [(ref[16 * k:16 * k + 8, :], ref[16 * k + 8:16 * k + 16, :]) for k in range(8)]
    low = [(ref[pl.ds(8 + a, 8, stride=16), :], ref[16 * (8 + a) + 8:16 * (8 + a) + 16, :]) for a in range(8)]
    return top + low


def sym_row(i, k):
    return 16 * k + i if (i >= 8 and k < 8) else 16 * i + k


def sym_product(left, right, emit):
    cols = right_factor(right)
    for i in range(16):
        lo = hi = None
        for k in range(16):
            s = bcast(left, sym_row(i, k))
            if i < 8:
                lo = s * cols[k][0] if lo is None else lo + s * cols[k][0]
            hi = s * cols[k][1] if hi is None else hi + s * cols[k][1]
        emit(i, lo, hi)


def analyse_tile(xin, t, idx_ref, yo_ref, ri_ref, rho, ob, xa, mref, yo, gp, bm, zm, tm, wa, st, write):
    lanes = pl.ds(pl.multiple_of(LANE * t, LANE), LANE)
    sub = lax.broadcasted_iota(jnp.int32, (8, LANE), 0)
    for v in range(8):
        rows = slice(8 * v, 8 * v + 8)
        vals = [xin[k, rows, lanes] for k in range(K)]
        total = vals[0]
        for k in range(1, K):
            total = total + vals[k]
        mean = total * (1.0 / K)
        mref[rows, :] = mean
        for k in range(K):
            xa[VARS * k + 8 * v:VARS * k + 8 * v + 8, :] = vals[k] - mean

    ob[0:32, :] = yo_ref[:, lanes]
    ob[32:64, :] = ri_ref[:, lanes]
    for p in range(32):
        col = idx_ref[p]
        y_lo = xa[pl.ds(col, 8, stride=VARS), :]
        y_hi = xa[pl.ds(col + 8 * VARS, 8, stride=VARS), :]
        prec = bcast(ob, 32 + p)
        yo[16 * p:16 * p + 8, :] = y_lo
        yo[16 * p + 8:16 * p + 16, :] = y_hi
        gp[16 * p:16 * p + 8, :] = y_lo * prec
        gp[16 * p + 8:16 * p + 16, :] = y_hi * prec
    g_lo = jnp.zeros((8, LANE), F32)
    g_hi = jnp.zeros((8, LANE), F32)
    for p in range(32):
        inno = bcast(ob, p) - bcast(mref, idx_ref[p])
        g_lo = g_lo + gp[16 * p:16 * p + 8, :] * inno
        g_hi = g_hi + gp[16 * p + 8:16 * p + 16, :] * inno
    diag = (K - 1) / rho
    trace = jnp.zeros((8, LANE), F32)
    for half in range(2):
        acc = [None] * 8
        acc2 = [None] * 8
        for p in range(32):
            y_lo = yo[16 * p:16 * p + 8, :]
            y_hi = yo[16 * p + 8:16 * p + 16, :]
            for r in range(8):
                s = bcast(gp, 16 * p + 8 * half + r)
                if half == 0:
                    acc[r] = s * y_lo if acc[r] is None else acc[r] + s * y_lo
                acc2[r] = s * y_hi if acc2[r] is None else acc2[r] + s * y_hi
        for r in range(8):
            i = 8 * half + r
            on = sub == r
            if half == 0:
                d = jnp.where(on, acc[r] + diag, acc[r])
                trace = trace + jnp.where(on, d, 0.0)
                bm[0, 16 * i:16 * i + 8, :] = d
                bm[0, 16 * i + 8:16 * i + 16, :] = acc2[r]
            else:
                d = jnp.where(on, acc2[r] + diag, acc2[r])
                trace = trace + jnp.where(on, d, 0.0)
                bm[0, 16 * i + 8:16 * i + 16, :] = d
    trace = jnp.broadcast_to(jnp.sum(trace, axis=0, keepdims=True), (8, LANE))
    inv = 1.0 / trace

    def slots(i):
        out = [(16 * i + 8, i >= 8)]
        if i < 8:
            out.append((16 * i, True))
        return out

    for i in range(16):
        for row, has_diag in slots(i):
            b = bm[0, row:row + 8, :] * inv
            bm[0, row:row + 8, :] = b
            z = b * -0.5
            if has_diag:
                z = jnp.where(sub == i % 8, z + 1.5, z)
            tm[row:row + 8, :] = z
            zm[0, row:row + 8, :] = z

    def emit_to(ref):
        def emit(i, lo, hi):
            if lo is not None:
                ref[16 * i:16 * i + 8, :] = lo
            ref[16 * i + 8:16 * i + 16, :] = hi
        return emit

    def emit_t(i, lo, hi):
        hi = hi * -0.5
        if lo is not None:
            lo = lo * -0.5
            tm[16 * i:16 * i + 8, :] = jnp.where(sub == i % 8, lo + 1.5, lo)
        else:
            hi = jnp.where(sub == i % 8, hi + 1.5, hi)
        tm[16 * i + 8:16 * i + 16, :] = hi

    def ns_step(step, carry):
        cur = lax.rem(step, 2)
        nxt = 1 - cur
        b_cur, b_nxt = bm.at[cur], bm.at[nxt]
        z_cur, z_nxt = zm.at[cur], zm.at[nxt]
        sym_product(b_cur, tm, emit_to(b_nxt))
        sym_product(z_cur, b_nxt, emit_t)
        sym_product(tm, z_cur, emit_to(z_nxt))
        return carry

    lax.fori_loop(0, NS_STEPS - 1, ns_step, 0)
    last = (NS_STEPS - 1) % 2
    z_fin = zm.at[last]

    root = 1.0 / jnp.sqrt(trace)
    cols = [(lo * root, hi * root) for lo, hi in right_factor(z_fin)]

    def sym_apply(lo, hi):
        gp[0:8, :] = lo
        gp[8:16, :] = hi
        a = b = None
        for k in range(16):
            s = bcast(gp, k)
            a = s * cols[k][0] if a is None else a + s * cols[k][0]
            b = s * cols[k][1] if b is None else b + s * cols[k][1]
        return a, b

    h_lo, h_hi = sym_apply(g_lo, g_hi)
    w_lo, w_hi = sym_apply(h_lo, h_hi)
    gp[0:8, :] = w_lo
    gp[8:16, :] = w_hi
    scale = math.sqrt(K - 1)
    for i in range(16):
        w = bcast(gp, i)
        wa[16 * i:16 * i + 8, :] = cols[i][0] * scale + w
        wa[16 * i + 8:16 * i + 16, :] = cols[i][1] * scale + w

    for v in range(0, 8, 2):
        xs = [(xa[VARS * i + 8 * v:VARS * i + 8 * v + 8, :], xa[VARS * i + 8 * v + 8:VARS * i + 8 * v + 16, :]) for i in range(K)]
        for k in range(K):
            a = mref[8 * v:8 * v + 8, :]
            b = mref[8 * v + 8:8 * v + 16, :]
            for i in range(K):
                s = bcast(wa, 16 * i + k)
                a = a + s * xs[i][0]
                b = b + s * xs[i][1]
            write(k, 8 * v, a, b)


def analysis_kernel(final, xin, idx_ref, yo_ref, ri_ref, rho_ref, out_ref, ob, xa, mref, yo, gp, bm, zm, tm, wa, st, send, recv):
    x, y, c = coords()
    greet()
    block = 4 * x + 2 * c + y

    if final:
        targets = [(r // 4, (r // 2) % 2, r % 2) for r in range(7, -1, -1)]
    else:
        targets = [(1, 1), (1, 0), (0, 1), (0, 0)]

    def ship(t, n):
        if final:
            dx, dy, dc = targets[n]
            x2, y2, c2 = (x + dx) % 2, (y + dy) % 2, (c + dc) % 2
            lane = pl.multiple_of(block * BLK + LANE * t, LANE)
            src = st.at[t, pl.ds(4 * (2 * x2 + c2), 4), pl.ds(pl.multiple_of(32 * y2, 32), 32), :]
            dst = out_ref.at[:, :, pl.ds(lane, LANE)]
            rsem = recv.at[t, block]
            is_self = n == len(targets) - 1
        else:
            dx, dy = targets[n]
            x2, y2, c2 = (x + dx) % 2, (y + dy) % 2, x
            lane = pl.multiple_of((2 * c + y) * BLK + LANE * t, LANE)
            src = st.at[t, pl.ds(4 * (2 * x2 + y2), 4), :, :]
            dst = out_ref.at[:, :, pl.ds(lane, LANE)]
            rsem = recv.at[t, 2 * c + y]
            is_self = (x == c) if n == len(targets) - 1 else False
        def local():
            return pltpu.make_async_copy(src, dst, rsem)

        def remote():
            return pltpu.make_async_remote_copy(src, dst, send.at[t, n], rsem, device_id=dev(x2, y2, c2), device_id_type=MESH)
        return is_self, local, remote

    def either(flag, yes, no):
        if flag is True:
            yes()
        elif flag is False:
            no()
        else:
            pl.when(flag)(yes)
            pl.when(jnp.logical_not(flag))(no)

    def tile(t, carry):
        def write(k, row, a, b):
            st[t, k, row:row + 8, :] = a
            st[t, k, row + 8:row + 16, :] = b
        analyse_tile(xin, t, idx_ref, yo_ref, ri_ref, rho_ref[0], ob, xa, mref, yo, gp, bm, zm, tm, wa, st, write)
        for n in range(len(targets)):
            is_self, local, remote = ship(t, n)
            either(is_self, lambda: local().start(), lambda: remote().start())
        return carry

    lax.fori_loop(0, TILES, tile, 0)
    for t in range(TILES):
        for n in range(len(targets)):
            is_self, local, remote = ship(t, n)
            either(is_self, lambda: None, lambda: remote().wait_send())
    for t in range(TILES):
        for s in range(8 if final else 4):
            lo = BLK * s + LANE * t
            await_bytes(out_ref.at[:, :, lo:lo + LANE], recv.at[t, s])


def analysis(state, obs_idx, obs_t, prec_t, rho, final):
    vm = pl.BlockSpec(memory_space=pltpu.VMEM)
    sm = pl.BlockSpec(memory_space=pltpu.SMEM)
    hbm = pl.BlockSpec(memory_space=pl.ANY)
    dma = pltpu.SemaphoreType.DMA
    out = (4, 32, COLS) if final else (4, VARS, HALF)
    peers = 8 if final else 4
    return pl.pallas_call(
        functools.partial(analysis_kernel, final),
        out_shape=jax.ShapeDtypeStruct(out, F32),
        in_specs=[vm, sm, vm, vm, sm],
        out_specs=hbm,
        scratch_shapes=[
            pltpu.VMEM((64, LANE), F32),
            pltpu.VMEM((K * VARS, LANE), F32),
            pltpu.VMEM((VARS, LANE), F32),
            pltpu.VMEM((512, LANE), F32),
            pltpu.VMEM((512, LANE), F32),
            pltpu.VMEM((2, 256, LANE), F32),
            pltpu.VMEM((2, 256, LANE), F32),
            pltpu.VMEM((256, LANE), F32),
            pltpu.VMEM((256, LANE), F32),
            pltpu.VMEM((TILES, K, VARS, LANE), F32),
            dma((TILES, peers)),
            dma((TILES, peers)),
        ],
        compiler_params=pltpu.CompilerParams(collective_id=4 if final else 3, has_side_effects=True, vmem_limit_bytes=32 * 1024 * 1024),
        name="analysis_last" if final else "analysis",
    )(state, obs_idx, obs_t, prec_t, rho)


def solution(mesh):
    def local_step(ens_local, mix_op, w_in, w_out, obs_val, obs_prec, obs_idx, inflation):
        cycles = obs_val.shape[0]
        ens_t = jnp.transpose(ens_local, (0, 2, 1))
        w_out_t = jnp.transpose(w_out, (0, 2, 1))
        obs_t = jnp.transpose(obs_val, (0, 2, 1))
        prec_t = jnp.transpose(obs_prec, (1, 0))
        ht, w_all, u_all = gather_state(ens_t, w_in, w_out_t)
        w_half = jnp.concatenate([w_all[0], w_all[1]], axis=2) * 0.5
        u_full = jnp.concatenate([u_all[0], u_all[1]], axis=2)
        w_pair = jnp.concatenate([jnp.pad(w_half, ((0, 0), (0, VARS), (0, 0))), jnp.pad(w_half, ((0, 0), (VARS, 0), (0, 0)))], axis=2)
        u_pair = jnp.concatenate([jnp.pad(u_full, ((0, 0), (0, VARS), (0, 0))), jnp.pad(u_full, ((0, 0), (VARS, 0), (0, 0)))], axis=2)
        u_pair = jnp.transpose(u_pair, (0, 2, 1))
        for cycle in range(cycles):
            final = cycle == cycles - 1
            state = forecast(ht.reshape(4 * VARS, HALF), mix_op, w_pair, u_pair)
            ht = analysis(state, obs_idx, obs_t[cycle], prec_t, inflation, final)
        return jnp.transpose(ht, (0, 2, 1))

    member_spec = P(("case", "ens"), None, "model")
    col_axes = ("case", "ens", "model")
    in_specs = (member_spec, P(None, None), P(None, None, "model"), P(None, "model", None), P(None, col_axes, None), P(col_axes, None), P(None), P(None))
    return jax.shard_map(local_step, mesh=mesh, in_specs=in_specs, out_specs=member_spec, check_vma=False)
```

```python
import functools
import math

import jax
import jax.numpy as jnp
from jax import lax
from jax.experimental import pallas as pl
from jax.experimental.pallas import tpu as pltpu
from jax.sharding import PartitionSpec as P

MESH = pl.DeviceIdType.MESH
K = 16
COLS = 5120
VARS = 64
HID = 1024
BLK = 640
LANE = 128
TILES = 5
ROWS = 512
HALF = 2560
NS_STEPS = 12
VMEM_LIMIT = 64 * 1024 * 1024 - 64 * 1024
F32 = jnp.float32
BF16 = jnp.bfloat16
C0 = math.sqrt(2.0 / math.pi)
C1 = 2.0 * C0
C2 = 8.0 * 0.044715 * C0


def coords():
    e = lax.axis_index("ens")
    return e // 2, lax.axis_index("model"), e % 2


def dev(x, y, c):
    return {"model": y, "ens": 2 * x + c}


def greet():
    x, y, c = coords()
    barrier = pltpu.get_barrier_semaphore()
    for r in range(1, 8):
        dx, dy, dc = r // 4, (r // 2) % 2, r % 2
        pl.semaphore_signal(barrier, inc=1, device_id=dev((x + dx) % 2, (y + dy) % 2, (c + dc) % 2), device_id_type=MESH)
    pl.semaphore_wait(barrier, 7)


def await_bytes(ref, sem):
    pltpu.make_async_copy(ref, ref, sem).wait()


def gather_kernel(ens_ref, w_ref, u_ref, out_ref, wall_ref, uall_ref, send, recv, wsend, wrecv, wloc):
    x, y, c = coords()
    greet()
    v0 = pl.multiple_of(32 * y, 32)

    def piece(h):
        return ens_ref.at[:, :, pl.ds(HALF * h, HALF)], out_ref.at[:, pl.ds(v0, 32), :]

    for h in range(2):
        src, dst = piece(h)
        own = jnp.logical_and(c == y, c == h)

        @pl.when(jnp.logical_not(own))
        def _():
            pltpu.make_async_remote_copy(src, dst, send.at[h], recv.at[y], device_id=dev(x, c, h), device_id_type=MESH).start()

        @pl.when(own)
        def _():
            pltpu.make_async_copy(src, dst, recv.at[y]).start()

    weights = ((w_ref, wall_ref), (u_ref, uall_ref))
    for n, (src, dst) in enumerate(weights):
        pltpu.make_async_remote_copy(src, dst.at[y], wsend.at[n], wrecv.at[n], device_id=dev(x, 1 - y, c), device_id_type=MESH).start()
        pltpu.make_async_copy(src, dst.at[y], wloc.at[n]).start()
    for n, (src, dst) in enumerate(weights):
        pltpu.make_async_copy(src, dst.at[y], wloc.at[n]).wait()
        pltpu.make_async_remote_copy(src, dst.at[1 - y], wsend.at[n], wrecv.at[n], device_id=dev(x, 1 - y, c), device_id_type=MESH).wait()
    for h in range(2):
        src, dst = piece(h)
        own = jnp.logical_and(c == y, c == h)

        @pl.when(jnp.logical_not(own))
        def _():
            pltpu.make_async_remote_copy(src, dst, send.at[h], recv.at[y], device_id=dev(x, c, h), device_id_type=MESH).wait_send()
    for s in range(2):
        await_bytes(out_ref.at[:, pl.ds(32 * s, 32), :], recv.at[s])


def gather_state(ens_t, w_in, w_out_t):
    vm = pl.BlockSpec(memory_space=pltpu.VMEM)
    hbm = pl.BlockSpec(memory_space=pl.ANY)
    dma = pltpu.SemaphoreType.DMA
    return pl.pallas_call(
        gather_kernel,
        out_shape=(
            jax.ShapeDtypeStruct((4, VARS, HALF), F32),
            jax.ShapeDtypeStruct((2,) + w_in.shape, BF16),
            jax.ShapeDtypeStruct((2,) + w_out_t.shape, BF16),
        ),
        in_specs=[vm, vm, vm],
        out_specs=(hbm, hbm, hbm),
        scratch_shapes=[dma((2,)), dma((2,)), dma((2,)), dma((2,)), dma((2,))],
        compiler_params=pltpu.CompilerParams(collective_id=1, has_side_effects=True, vmem_limit_bytes=16 * 1024 * 1024),
        name="gather_state",
    )(ens_t, w_in, w_out_t)


def forecast_kernel(layers, ht_ref, a_ref, w_ref, u_ref, out_ref, a_vm, hb, hf, mt, st, a_sem, xsend, xrecv, send, recv):
    x, y, c = coords()
    partner = dev(x, y, 1 - c)
    greet()

    def a_copy(t, q):
        row = pl.multiple_of((4 * c + q) * BLK + LANE * t, LANE)
        return pltpu.make_async_copy(a_ref.at[pl.ds(row, LANE), :], a_vm.at[t, pl.ds(LANE * q, LANE), :], a_sem.at[t, q])

    for t in range(TILES):
        for q in range(4):
            a_copy(t, q).start()

    def share(buf, t):
        lane = pl.multiple_of(LANE * t, LANE)
        piece = hb.at[buf, pl.ds(4 * c, 4), pl.ds(lane, LANE), :]
        return pltpu.make_async_remote_copy(piece, piece, xsend.at[buf, t], xrecv.at[buf, t], device_id=partner, device_id_type=MESH)

    for t in range(TILES):
        for q in range(4):
            part = ht_ref[:, BLK * q + LANE * t:BLK * q + LANE * (t + 1)].T
            hf[t, LANE * q:LANE * (q + 1), :] = part
            hb[0, 4 * c + q, LANE * t:LANE * (t + 1), :] = part.astype(BF16)
        share(0, t).start()

    def await_share(buf, t):
        lane = pl.multiple_of(LANE * t, LANE)
        await_bytes(hb.at[buf, pl.ds(4 * (1 - c), 4), pl.ds(lane, LANE), :], xrecv.at[buf, t])

    own_half = x == c
    mine = 4 * (2 * x + y)

    def ship(t, q):
        c2, y2 = q // 2, q % 2
        lane = pl.multiple_of(LANE * t, LANE)
        src = st.at[t, :, :, pl.ds(LANE * q, LANE)]
        dst = out_ref.at[pl.ds(mine, 4), :, pl.ds(lane, LANE)]
        is_self = jnp.logical_and(own_half, jnp.logical_and(c == c2, y == y2))
        rsem = recv.at[t, 2 * x + y]
        def local():
            return pltpu.make_async_copy(src, dst, rsem)

        def remote():
            return pltpu.make_async_remote_copy(src, dst, send.at[t, q], rsem, device_id=dev(c, y2, c2), device_id_type=MESH)
        return is_self, local, remote

    def layer_body(layer, carry):
        cur = lax.rem(layer, 2)
        nxt = 1 - cur
        for t in range(TILES):
            await_share(cur, t)
            share(cur, t).wait_send()

        def tile_body(t, carry2):
            @pl.when(layer == 0)
            def _():
                for q in range(4):
                    a_copy(t, q).wait()
            state = hb[cur].reshape(COLS, 4 * VARS)
            for r in range(2):
                mixed = jnp.dot(a_vm[t, 256 * r:256 * (r + 1), :], state, preferred_element_type=F32)
                mt[256 * r:256 * (r + 1), :] = mixed.astype(BF16)
            sums = [None, None]
            for n in range(8):
                for p in range(2):
                    h = jnp.dot(mt[:, 128 * p:128 * (p + 1)], w_ref[layer, :, 256 * n:256 * (n + 1)], preferred_element_type=F32)
                    z = h * (C1 + C2 * (h * h))
                    q_act = (h + h * jnp.tanh(z)).astype(BF16)
                    part = jnp.dot(q_act, u_ref[layer, 256 * n:256 * (n + 1), :], preferred_element_type=F32)
                    sums[p] = part if sums[p] is None else sums[p] + part
            for p in range(2):
                hf[t, :, 128 * p:128 * (p + 1)] = hf[t, :, 128 * p:128 * (p + 1)] + sums[p]

            @pl.when(layer < layers - 1)
            def _():
                lane = pl.multiple_of(LANE * t, LANE)
                for q in range(4):
                    hb[nxt, 4 * c + q, pl.ds(lane, LANE), :] = hf[t, LANE * q:LANE * (q + 1), :].astype(BF16)
                share(nxt, t).start()

            @pl.when(layer == layers - 1)
            def _():
                for q in range(4):
                    st[t, :, :, LANE * q:LANE * (q + 1)] = hf[t, LANE * q:LANE * (q + 1), :].T.reshape(4, VARS, LANE)
                for q in range(4):
                    is_self, local, remote = ship(t, q)

                    @pl.when(is_self)
                    def _():
                        local().start()

                    @pl.when(jnp.logical_not(is_self))
                    def _():
                        remote().start()
            return carry2

        return lax.fori_loop(0, TILES, tile_body, carry)

    lax.fori_loop(0, layers, layer_body, 0)

    for t in range(TILES):
        for q in range(4):
            is_self, local, remote = ship(t, q)

            @pl.when(jnp.logical_not(is_self))
            def _():
                remote().wait_send()
    for t in range(TILES):
        for s in range(4):
            await_bytes(out_ref.at[4 * s:4 * s + 4, :, LANE * t:LANE * (t + 1)], recv.at[t, s])


def forecast(ht, mix_op, w_pair, u_pair):
    vm = pl.BlockSpec(memory_space=pltpu.VMEM)
    hbm = pl.BlockSpec(memory_space=pl.ANY)
    dma = pltpu.SemaphoreType.DMA
    layers = w_pair.shape[0]
    return pl.pallas_call(
        functools.partial(forecast_kernel, layers),
        out_shape=jax.ShapeDtypeStruct((K, VARS, BLK), F32),
        in_specs=[vm, hbm, vm, vm],
        out_specs=hbm,
        scratch_shapes=[
            pltpu.VMEM((TILES, ROWS, COLS), BF16),
            pltpu.VMEM((2, 8, BLK, 4 * VARS), BF16),
            pltpu.VMEM((TILES, ROWS, 4 * VARS), F32),
            pltpu.VMEM((ROWS, 4 * VARS), BF16),
            pltpu.VMEM((TILES, 4, VARS, ROWS), F32),
            dma((TILES, 4)),
            dma((2, TILES)),
            dma((2, TILES)),
            dma((TILES, 4)),
            dma((TILES, 4)),
        ],
        compiler_params=pltpu.CompilerParams(collective_id=2, has_side_effects=True, vmem_limit_bytes=VMEM_LIMIT),
        name="forecast",
    )(ht, mix_op, w_pair, u_pair)


def bcast(ref, row):
    return ref[pl.ds(row, 8, stride=0), :]


def right_factor(ref):
    top = [(ref[16 * k:16 * k + 8, :], ref[16 * k + 8:16 * k + 16, :]) for k in range(8)]
    low = [(ref[pl.ds(8 + a, 8, stride=16), :], ref[16 * (8 + a) + 8:16 * (8 + a) + 16, :]) for a in range(8)]
    return top + low


def sym_row(i, k):
    return 16 * k + i if (i >= 8 and k < 8) else 16 * i + k


def sym_product(left, right, emit):
    cols = right_factor(right)
    for i in range(16):
        lo = hi = None
        for k in range(16):
            s = bcast(left, sym_row(i, k))
            if i < 8:
                lo = s * cols[k][0] if lo is None else lo + s * cols[k][0]
            hi = s * cols[k][1] if hi is None else hi + s * cols[k][1]
        emit(i, lo, hi)


def analyse_tile(xin, t, idx_ref, yo_ref, ri_ref, rho, ob, xa, mref, yo, gp, bm, zm, tm, wa, st, write):
    lanes = pl.ds(pl.multiple_of(LANE * t, LANE), LANE)
    sub = lax.broadcasted_iota(jnp.int32, (8, LANE), 0)
    for v in range(8):
        rows = slice(8 * v, 8 * v + 8)
        vals = [xin[k, rows, lanes] for k in range(K)]
        total = vals[0]
        for k in range(1, K):
            total = total + vals[k]
        mean = total * (1.0 / K)
        mref[rows, :] = mean
        for k in range(K):
            xa[VARS * k + 8 * v:VARS * k + 8 * v + 8, :] = vals[k] - mean

    ob[0:32, :] = yo_ref[:, lanes]
    ob[32:64, :] = ri_ref[:, lanes]
    for p in range(32):
        col = idx_ref[p]
        y_lo = xa[pl.ds(col, 8, stride=VARS), :]
        y_hi = xa[pl.ds(col + 8 * VARS, 8, stride=VARS), :]
        prec = bcast(ob, 32 + p)
        yo[16 * p:16 * p + 8, :] = y_lo
        yo[16 * p + 8:16 * p + 16, :] = y_hi
        gp[16 * p:16 * p + 8, :] = y_lo * prec
        gp[16 * p + 8:16 * p + 16, :] = y_hi * prec
    g_lo = jnp.zeros((8, LANE), F32)
    g_hi = jnp.zeros((8, LANE), F32)
    for p in range(32):
        inno = bcast(ob, p) - bcast(mref, idx_ref[p])
        g_lo = g_lo + gp[16 * p:16 * p + 8, :] * inno
        g_hi = g_hi + gp[16 * p + 8:16 * p + 16, :] * inno
    diag = (K - 1) / rho
    trace = jnp.zeros((8, LANE), F32)
    for half in range(2):
        acc = [None] * 8
        acc2 = [None] * 8
        for p in range(32):
            y_lo = yo[16 * p:16 * p + 8, :]
            y_hi = yo[16 * p + 8:16 * p + 16, :]
            for r in range(8):
                s = bcast(gp, 16 * p + 8 * half + r)
                if half == 0:
                    acc[r] = s * y_lo if acc[r] is None else acc[r] + s * y_lo
                acc2[r] = s * y_hi if acc2[r] is None else acc2[r] + s * y_hi
        for r in range(8):
            i = 8 * half + r
            on = sub == r
            if half == 0:
                d = jnp.where(on, acc[r] + diag, acc[r])
                trace = trace + jnp.where(on, d, 0.0)
                bm[0, 16 * i:16 * i + 8, :] = d
                bm[0, 16 * i + 8:16 * i + 16, :] = acc2[r]
            else:
                d = jnp.where(on, acc2[r] + diag, acc2[r])
                trace = trace + jnp.where(on, d, 0.0)
                bm[0, 16 * i + 8:16 * i + 16, :] = d
    trace = jnp.broadcast_to(jnp.sum(trace, axis=0, keepdims=True), (8, LANE))
    inv = 1.0 / trace

    def slots(i):
        out = [(16 * i + 8, i >= 8)]
        if i < 8:
            out.append((16 * i, True))
        return out

    for i in range(16):
        for row, has_diag in slots(i):
            b = bm[0, row:row + 8, :] * inv
            bm[0, row:row + 8, :] = b
            z = b * -0.5
            if has_diag:
                z = jnp.where(sub == i % 8, z + 1.5, z)
            tm[row:row + 8, :] = z
            zm[0, row:row + 8, :] = z

    def emit_to(ref):
        def emit(i, lo, hi):
            if lo is not None:
                ref[16 * i:16 * i + 8, :] = lo
            ref[16 * i + 8:16 * i + 16, :] = hi
        return emit

    def emit_t(i, lo, hi):
        hi = hi * -0.5
        if lo is not None:
            lo = lo * -0.5
            tm[16 * i:16 * i + 8, :] = jnp.where(sub == i % 8, lo + 1.5, lo)
        else:
            hi = jnp.where(sub == i % 8, hi + 1.5, hi)
        tm[16 * i + 8:16 * i + 16, :] = hi

    def ns_step(step, carry):
        cur = lax.rem(step, 2)
        nxt = 1 - cur
        b_cur, b_nxt = bm.at[cur], bm.at[nxt]
        z_cur, z_nxt = zm.at[cur], zm.at[nxt]
        sym_product(b_cur, tm, emit_to(b_nxt))
        sym_product(z_cur, b_nxt, emit_t)
        sym_product(tm, z_cur, emit_to(z_nxt))
        return carry

    lax.fori_loop(0, NS_STEPS - 1, ns_step, 0)
    last = (NS_STEPS - 1) % 2
    z_fin = zm.at[last]

    root = 1.0 / jnp.sqrt(trace)
    cols = [(lo * root, hi * root) for lo, hi in right_factor(z_fin)]

    def sym_apply(lo, hi):
        gp[0:8, :] = lo
        gp[8:16, :] = hi
        a = b = None
        for k in range(16):
            s = bcast(gp, k)
            a = s * cols[k][0] if a is None else a + s * cols[k][0]
            b = s * cols[k][1] if b is None else b + s * cols[k][1]
        return a, b

    h_lo, h_hi = sym_apply(g_lo, g_hi)
    w_lo, w_hi = sym_apply(h_lo, h_hi)
    gp[0:8, :] = w_lo
    gp[8:16, :] = w_hi
    scale = math.sqrt(K - 1)
    for i in range(16):
        w = bcast(gp, i)
        wa[16 * i:16 * i + 8, :] = cols[i][0] * scale + w
        wa[16 * i + 8:16 * i + 16, :] = cols[i][1] * scale + w

    for v in range(0, 8, 2):
        xs = [(xa[VARS * i + 8 * v:VARS * i + 8 * v + 8, :], xa[VARS * i + 8 * v + 8:VARS * i + 8 * v + 16, :]) for i in range(K)]
        for k in range(K):
            a = mref[8 * v:8 * v + 8, :]
            b = mref[8 * v + 8:8 * v + 16, :]
            for i in range(K):
                s = bcast(wa, 16 * i + k)
                a = a + s * xs[i][0]
                b = b + s * xs[i][1]
            write(k, 8 * v, a, b)


def analysis_kernel(final, xin, idx_ref, yo_ref, ri_ref, rho_ref, out_ref, ob, xa, mref, yo, gp, bm, zm, tm, wa, st, send, recv):
    x, y, c = coords()
    greet()
    block = 4 * x + 2 * c + y

    if final:
        targets = [(r // 4, (r // 2) % 2, r % 2) for r in range(7, -1, -1)]
    else:
        targets = [(1, 1), (1, 0), (0, 1), (0, 0)]

    def ship(t, n):
        if final:
            dx, dy, dc = targets[n]
            x2, y2, c2 = (x + dx) % 2, (y + dy) % 2, (c + dc) % 2
            lane = pl.multiple_of(block * BLK + LANE * t, LANE)
            src = st.at[t, pl.ds(4 * (2 * x2 + c2), 4), pl.ds(pl.multiple_of(32 * y2, 32), 32), :]
            dst = out_ref.at[:, :, pl.ds(lane, LANE)]
            rsem = recv.at[t, block]
            is_self = n == len(targets) - 1
        else:
            dx, dy = targets[n]
            x2, y2, c2 = (x + dx) % 2, (y + dy) % 2, x
            lane = pl.multiple_of((2 * c + y) * BLK + LANE * t, LANE)
            src = st.at[t, pl.ds(4 * (2 * x2 + y2), 4), :, :]
            dst = out_ref.at[:, :, pl.ds(lane, LANE)]
            rsem = recv.at[t, 2 * c + y]
            is_self = (x == c) if n == len(targets) - 1 else False
        def local():
            return pltpu.make_async_copy(src, dst, rsem)

        def remote():
            return pltpu.make_async_remote_copy(src, dst, send.at[t, n], rsem, device_id=dev(x2, y2, c2), device_id_type=MESH)
        return is_self, local, remote

    def either(flag, yes, no):
        if flag is True:
            yes()
        elif flag is False:
            no()
        else:
            pl.when(flag)(yes)
            pl.when(jnp.logical_not(flag))(no)

    def tile(t, carry):
        def write(k, row, a, b):
            st[t, k, row:row + 8, :] = a
            st[t, k, row + 8:row + 16, :] = b
        analyse_tile(xin, t, idx_ref, yo_ref, ri_ref, rho_ref[0], ob, xa, mref, yo, gp, bm, zm, tm, wa, st, write)
        for n in range(len(targets)):
            is_self, local, remote = ship(t, n)
            either(is_self, lambda: local().start(), lambda: remote().start())
        return carry

    lax.fori_loop(0, TILES, tile, 0)
    for t in range(TILES):
        for n in range(len(targets)):
            is_self, local, remote = ship(t, n)
            either(is_self, lambda: None, lambda: remote().wait_send())
    for t in range(TILES):
        for s in range(8 if final else 4):
            lo = BLK * s + LANE * t
            await_bytes(out_ref.at[:, :, lo:lo + LANE], recv.at[t, s])


def analysis(state, obs_idx, obs_t, prec_t, rho, final):
    vm = pl.BlockSpec(memory_space=pltpu.VMEM)
    sm = pl.BlockSpec(memory_space=pltpu.SMEM)
    hbm = pl.BlockSpec(memory_space=pl.ANY)
    dma = pltpu.SemaphoreType.DMA
    out = (4, 32, COLS) if final else (4, VARS, HALF)
    peers = 8 if final else 4
    return pl.pallas_call(
        functools.partial(analysis_kernel, final),
        out_shape=jax.ShapeDtypeStruct(out, F32),
        in_specs=[vm, sm, vm, vm, sm],
        out_specs=hbm,
        scratch_shapes=[
            pltpu.VMEM((64, LANE), F32),
            pltpu.VMEM((K * VARS, LANE), F32),
            pltpu.VMEM((VARS, LANE), F32),
            pltpu.VMEM((512, LANE), F32),
            pltpu.VMEM((512, LANE), F32),
            pltpu.VMEM((2, 256, LANE), F32),
            pltpu.VMEM((2, 256, LANE), F32),
            pltpu.VMEM((256, LANE), F32),
            pltpu.VMEM((256, LANE), F32),
            pltpu.VMEM((TILES, K, VARS, LANE), F32),
            dma((TILES, peers)),
            dma((TILES, peers)),
        ],
        compiler_params=pltpu.CompilerParams(collective_id=4 if final else 3, has_side_effects=True, vmem_limit_bytes=32 * 1024 * 1024),
        name="analysis_last" if final else "analysis",
    )(state, obs_idx, obs_t, prec_t, rho)


def solution(mesh):
    def local_step(ens_local, mix_op, w_in, w_out, obs_val, obs_prec, obs_idx, inflation):
        cycles = obs_val.shape[0]
        ens_t = jnp.transpose(ens_local, (0, 2, 1))
        w_out_t = jnp.transpose(w_out, (0, 2, 1))
        obs_t = jnp.transpose(obs_val, (0, 2, 1))
        prec_t = jnp.transpose(obs_prec, (1, 0))
        ht, w_all, u_all = gather_state(ens_t, w_in, w_out_t)
        w_half = jnp.concatenate([w_all[0], w_all[1]], axis=2) * 0.5
        u_full = jnp.concatenate([u_all[0], u_all[1]], axis=2)
        w_pair = jnp.concatenate([jnp.pad(w_half, ((0, 0), (0, VARS), (0, 0))), jnp.pad(w_half, ((0, 0), (VARS, 0), (0, 0)))], axis=2)
        u_pair = jnp.concatenate([jnp.pad(u_full, ((0, 0), (0, VARS), (0, 0))), jnp.pad(u_full, ((0, 0), (VARS, 0), (0, 0)))], axis=2)
        u_pair = jnp.transpose(u_pair, (0, 2, 1))
        for cycle in range(cycles):
            final = cycle == cycles - 1
            state = forecast(ht.reshape(4 * VARS, HALF), mix_op, w_pair, u_pair)
            ht = analysis(state, obs_idx, obs_t[cycle], prec_t, inflation, final)
        return jnp.transpose(ht, (0, 2, 1))

    member_spec = P(("case", "ens"), None, "model")
    col_axes = ("case", "ens", "model")
    in_specs = (member_spec, P(None, None), P(None, None, "model"), P(None, "model", None), P(None, col_axes, None), P(col_axes, None), P(None), P(None))
    return jax.shard_map(local_step, mesh=mesh, in_specs=in_specs, out_specs=member_spec, check_vma=False)
```

```python
import functools
import math

import jax
import jax.numpy as jnp
from jax import lax
from jax.experimental import pallas as pl
from jax.experimental.pallas import tpu as pltpu
from jax.sharding import PartitionSpec as P

MESH = pl.DeviceIdType.MESH
K = 16
COLS = 5120
VARS = 64
HID = 1024
BLK = 640
LANE = 128
TILES = 5
ROWS = 512
HALF = 2560
NS_STEPS = 12
VMEM_LIMIT = 64 * 1024 * 1024 - 64 * 1024
F32 = jnp.float32
BF16 = jnp.bfloat16
C0 = math.sqrt(2.0 / math.pi)
C1 = 2.0 * C0
C2 = 8.0 * 0.044715 * C0


def coords():
    e = lax.axis_index("ens")
    return e // 2, lax.axis_index("model"), e % 2


def dev(x, y, c):
    return {"model": y, "ens": 2 * x + c}


def greet():
    x, y, c = coords()
    barrier = pltpu.get_barrier_semaphore()
    for r in range(1, 8):
        dx, dy, dc = r // 4, (r // 2) % 2, r % 2
        pl.semaphore_signal(barrier, inc=1, device_id=dev((x + dx) % 2, (y + dy) % 2, (c + dc) % 2), device_id_type=MESH)
    pl.semaphore_wait(barrier, 7)


def await_bytes(ref, sem):
    pltpu.make_async_copy(ref, ref, sem).wait()


def bcast(ref, row):
    return ref[pl.ds(row, 8, stride=0), :]


def right_factor(ref):
    top = [(ref[16 * k:16 * k + 8, :], ref[16 * k + 8:16 * k + 16, :]) for k in range(8)]
    low = [(ref[pl.ds(8 + a, 8, stride=16), :], ref[16 * (8 + a) + 8:16 * (8 + a) + 16, :]) for a in range(8)]
    return top + low


def sym_row(i, k):
    return 16 * k + i if (i >= 8 and k < 8) else 16 * i + k


def sym_product(left, right, emit):
    cols = right_factor(right)
    for i in range(16):
        lo = hi = None
        for k in range(16):
            s = bcast(left, sym_row(i, k))
            if i < 8:
                lo = s * cols[k][0] if lo is None else lo + s * cols[k][0]
            hi = s * cols[k][1] if hi is None else hi + s * cols[k][1]
        emit(i, lo, hi)


def analyse_tile(xin, t, idx_ref, yo_ref, ri_ref, rho, ob, xa, mref, yo, gp, bm, zm, tm, wa, write):
    lanes = pl.ds(pl.multiple_of(LANE * t, LANE), LANE)
    sub = lax.broadcasted_iota(jnp.int32, (8, LANE), 0)
    for v in range(8):
        rows = slice(8 * v, 8 * v + 8)
        vals = [xin[k, rows, lanes] for k in range(K)]
        total = vals[0]
        for k in range(1, K):
            total = total + vals[k]
        mean = total * (1.0 / K)
        mref[rows, :] = mean
        for k in range(K):
            xa[VARS * k + 8 * v:VARS * k + 8 * v + 8, :] = vals[k] - mean

    ob[0:32, :] = yo_ref[:, lanes]
    ob[32:64, :] = ri_ref[:, lanes]
    for p in range(32):
        col = idx_ref[p]
        y_lo = xa[pl.ds(col, 8, stride=VARS), :]
        y_hi = xa[pl.ds(col + 8 * VARS, 8, stride=VARS), :]
        prec = bcast(ob, 32 + p)
        yo[16 * p:16 * p + 8, :] = y_lo
        yo[16 * p + 8:16 * p + 16, :] = y_hi
        gp[16 * p:16 * p + 8, :] = y_lo * prec
        gp[16 * p + 8:16 * p + 16, :] = y_hi * prec
    g_lo = jnp.zeros((8, LANE), F32)
    g_hi = jnp.zeros((8, LANE), F32)
    for p in range(32):
        inno = bcast(ob, p) - bcast(mref, idx_ref[p])
        g_lo = g_lo + gp[16 * p:16 * p + 8, :] * inno
        g_hi = g_hi + gp[16 * p + 8:16 * p + 16, :] * inno
    diag = (K - 1) / rho
    trace = jnp.zeros((8, LANE), F32)
    for half in range(2):
        acc = [None] * 8
        acc2 = [None] * 8
        for p in range(32):
            y_lo = yo[16 * p:16 * p + 8, :]
            y_hi = yo[16 * p + 8:16 * p + 16, :]
            for r in range(8):
                s = bcast(gp, 16 * p + 8 * half + r)
                if half == 0:
                    acc[r] = s * y_lo if acc[r] is None else acc[r] + s * y_lo
                acc2[r] = s * y_hi if acc2[r] is None else acc2[r] + s * y_hi
        for r in range(8):
            i = 8 * half + r
            on = sub == r
            if half == 0:
                d = jnp.where(on, acc[r] + diag, acc[r])
                trace = trace + jnp.where(on, d, 0.0)
                bm[0, 16 * i:16 * i + 8, :] = d
                bm[0, 16 * i + 8:16 * i + 16, :] = acc2[r]
            else:
                d = jnp.where(on, acc2[r] + diag, acc2[r])
                trace = trace + jnp.where(on, d, 0.0)
                bm[0, 16 * i + 8:16 * i + 16, :] = d
    trace = jnp.broadcast_to(jnp.sum(trace, axis=0, keepdims=True), (8, LANE))
    inv = 1.0 / trace

    def slots(i):
        out = [(16 * i + 8, i >= 8)]
        if i < 8:
            out.append((16 * i, True))
        return out

    for i in range(16):
        for row, has_diag in slots(i):
            b = bm[0, row:row + 8, :] * inv
            bm[0, row:row + 8, :] = b
            z = b * -0.5
            if has_diag:
                z = jnp.where(sub == i % 8, z + 1.5, z)
            tm[row:row + 8, :] = z
            zm[0, row:row + 8, :] = z

    def emit_to(ref):
        def emit(i, lo, hi):
            if lo is not None:
                ref[16 * i:16 * i + 8, :] = lo
            ref[16 * i + 8:16 * i + 16, :] = hi
        return emit

    def emit_t(i, lo, hi):
        hi = hi * -0.5
        if lo is not None:
            lo = lo * -0.5
            tm[16 * i:16 * i + 8, :] = jnp.where(sub == i % 8, lo + 1.5, lo)
        else:
            hi = jnp.where(sub == i % 8, hi + 1.5, hi)
        tm[16 * i + 8:16 * i + 16, :] = hi

    def ns_step(step, carry):
        cur = lax.rem(step, 2)
        nxt = 1 - cur
        b_cur, b_nxt = bm.at[cur], bm.at[nxt]
        z_cur, z_nxt = zm.at[cur], zm.at[nxt]
        sym_product(b_cur, tm, emit_to(b_nxt))
        sym_product(z_cur, b_nxt, emit_t)
        sym_product(tm, z_cur, emit_to(z_nxt))
        return carry

    lax.fori_loop(0, NS_STEPS - 1, ns_step, 0)
    last = (NS_STEPS - 1) % 2
    z_fin = zm.at[last]

    root = 1.0 / jnp.sqrt(trace)
    cols = [(lo * root, hi * root) for lo, hi in right_factor(z_fin)]

    def sym_apply(lo, hi):
        gp[0:8, :] = lo
        gp[8:16, :] = hi
        a = b = None
        for k in range(16):
            s = bcast(gp, k)
            a = s * cols[k][0] if a is None else a + s * cols[k][0]
            b = s * cols[k][1] if b is None else b + s * cols[k][1]
        return a, b

    h_lo, h_hi = sym_apply(g_lo, g_hi)
    w_lo, w_hi = sym_apply(h_lo, h_hi)
    gp[0:8, :] = w_lo
    gp[8:16, :] = w_hi
    scale = math.sqrt(K - 1)
    for i in range(16):
        w = bcast(gp, i)
        wa[16 * i:16 * i + 8, :] = cols[i][0] * scale + w
        wa[16 * i + 8:16 * i + 16, :] = cols[i][1] * scale + w

    for v in range(0, 8, 2):
        xs = [(xa[VARS * i + 8 * v:VARS * i + 8 * v + 8, :], xa[VARS * i + 8 * v + 8:VARS * i + 8 * v + 16, :]) for i in range(K)]
        for k in range(K):
            a = mref[8 * v:8 * v + 8, :]
            b = mref[8 * v + 8:8 * v + 16, :]
            for i in range(K):
                s = bcast(wa, 16 * i + k)
                a = a + s * xs[i][0]
                b = b + s * xs[i][1]
            write(k, 8 * v, a, b)


def either(flag, yes, no):
    if flag is True:
        yes()
    elif flag is False:
        no()
    else:
        pl.when(flag)(yes)
        pl.when(jnp.logical_not(flag))(no)


def cycle_kernel(layers, cycles, ens_ref, win_ref, wout_ref, a_ref, obs_ref, prec_ref, idx_ref, rho_ref, out_ref,
                 a_vm, hb, hf, mt, st, ht, xin, gst, wr, ur, wp, up,
                 ob, xa, mref, yo, gp, bm, zm, tm, wa,
                 a_sem, isend, irecv, wsend, wrecv, xsend, xrecv, fsend, frecv, gsend, grecv, osend, orecv):
    x, y, c = coords()
    partner = dev(x, y, 1 - c)
    greet()

    def init_piece(h):
        src = ens_ref.at[:, :, pl.ds(HALF * h, HALF)]
        dst = ht.at[:, pl.ds(pl.multiple_of(32 * y, 32), 32), :]
        is_self = jnp.logical_and(c == y, c == h)

        def local():
            return pltpu.make_async_copy(src, dst, irecv.at[y])

        def remote():
            return pltpu.make_async_remote_copy(src, dst, isend.at[h], irecv.at[y], device_id=dev(x, c, h), device_id_type=MESH)
        return is_self, local, remote

    weights = ((win_ref, wr), (wout_ref, ur))

    def weight_remote(n):
        src, dst = weights[n]
        return pltpu.make_async_remote_copy(src, dst.at[y], wsend.at[n], wrecv.at[n, 0], device_id=dev(x, 1 - y, c), device_id_type=MESH)

    def weight_local(n):
        src, dst = weights[n]
        return pltpu.make_async_copy(src, dst.at[y], wrecv.at[n, 1])

    for n in range(2):
        weight_remote(n).start()
        weight_local(n).start()
    for h in range(2):
        is_self, local, remote = init_piece(h)
        either(is_self, lambda: local().start(), lambda: remote().start())

    def a_copy(t, q):
        row = pl.multiple_of((4 * c + q) * BLK + LANE * t, LANE)
        return pltpu.make_async_copy(a_ref.at[pl.ds(row, LANE), :], a_vm.at[t, pl.ds(LANE * q, LANE), :], a_sem.at[t, q])

    for t in range(TILES):
        for q in range(4):
            a_copy(t, q).start()

    for n in range(2):
        weight_local(n).wait()
        weight_remote(n).wait()
    for layer in range(layers):
        for part in range(2):
            for p in range(2):
                lo = HID * p + 512 * part
                wv = (wr[part, layer].astype(F32) * 0.5).astype(BF16)
                wz = jnp.zeros_like(wv)
                wp[layer, :, lo:lo + 512] = jnp.concatenate([wv, wz] if p == 0 else [wz, wv], axis=0)
                uv = ur[part, layer].astype(F32)
                uz = jnp.zeros_like(uv)
                up[layer, lo:lo + 512, :] = jnp.concatenate([uv, uz] if p == 0 else [uz, uv], axis=0).T.astype(BF16)

    def share(buf, t):
        lane = pl.multiple_of(LANE * t, LANE)
        piece = hb.at[buf, pl.ds(4 * c, 4), pl.ds(lane, LANE), :]
        return pltpu.make_async_remote_copy(piece, piece, xsend.at[buf, t], xrecv.at[buf, t], device_id=partner, device_id_type=MESH)

    def await_share(buf, t):
        lane = pl.multiple_of(LANE * t, LANE)
        await_bytes(hb.at[buf, pl.ds(4 * (1 - c), 4), pl.ds(lane, LANE), :], xrecv.at[buf, t])

    mine = 4 * (2 * x + y)

    def f_ship(t, q):
        c2, y2 = q // 2, q % 2
        lane = pl.multiple_of(LANE * t, LANE)
        src = st.at[t, :, :, pl.ds(LANE * q, LANE)]
        dst = xin.at[pl.ds(mine, 4), :, pl.ds(lane, LANE)]
        is_self = jnp.logical_and(x == c, jnp.logical_and(c == c2, y == y2))
        rsem = frecv.at[t, 2 * x + y]

        def local():
            return pltpu.make_async_copy(src, dst, rsem)

        def remote():
            return pltpu.make_async_remote_copy(src, dst, fsend.at[t, q], rsem, device_id=dev(c, y2, c2), device_id_type=MESH)
        return is_self, local, remote

    block = 4 * x + 2 * c + y
    back = [(1, 1), (1, 0), (0, 1), (0, 0)]

    def g_ship(t, n):
        dx, dy = back[n]
        x2, y2 = (x + dx) % 2, (y + dy) % 2
        lane = pl.multiple_of((2 * c + y) * BLK + LANE * t, LANE)
        src = gst.at[t, pl.ds(4 * (2 * x2 + y2), 4), :, :]
        dst = ht.at[:, :, pl.ds(lane, LANE)]
        rsem = grecv.at[t, 2 * c + y]
        is_self = (x == c) if n == 3 else False

        def local():
            return pltpu.make_async_copy(src, dst, rsem)

        def remote():
            return pltpu.make_async_remote_copy(src, dst, gsend.at[t, n], rsem, device_id=dev(x2, y2, x), device_id_type=MESH)
        return is_self, local, remote

    def o_ship(t, n):
        r = 7 - n
        x2, y2, c2 = (x + r // 4) % 2, (y + (r // 2) % 2) % 2, (c + r % 2) % 2
        lane = pl.multiple_of(block * BLK + LANE * t, LANE)
        src = gst.at[t, pl.ds(4 * (2 * x2 + c2), 4), pl.ds(pl.multiple_of(32 * y2, 32), 32), :]
        dst = out_ref.at[:, :, pl.ds(lane, LANE)]
        rsem = orecv.at[t, block]

        def local():
            return pltpu.make_async_copy(src, dst, rsem)

        def remote():
            return pltpu.make_async_remote_copy(src, dst, osend.at[t, n], rsem, device_id=dev(x2, y2, c2), device_id_type=MESH)
        return r == 0, local, remote

    def start(ship):
        is_self, local, remote = ship
        either(is_self, lambda: local().start(), lambda: remote().start())

    def sent(ship):
        is_self, local, remote = ship
        either(is_self, lambda: None, lambda: remote().wait_send())

    def cycle_body(cycle, carry):
        first = lax.rem(cycle * layers, 2)

        @pl.when(cycle == 0)
        def _():
            for h in range(2):
                sent(init_piece(h))
            for s in range(2):
                await_bytes(ht.at[:, 32 * s:32 * s + 32, :], irecv.at[s])

        def load_body(t, carry2):
            @pl.when(cycle > 0)
            def _():
                for s in range(4):
                    await_bytes(ht.at[:, :, pl.ds(pl.multiple_of(BLK * s + LANE * t, LANE), LANE)], grecv.at[t, s])
            lane = pl.multiple_of(LANE * t, LANE)
            for q in range(4):
                part = ht[:, :, pl.ds(pl.multiple_of(BLK * q + lane, LANE), LANE)].reshape(4 * VARS, LANE).T
                hf[t, LANE * q:LANE * (q + 1), :] = part
                hb[first, 4 * c + q, pl.ds(lane, LANE), :] = part.astype(BF16)
            share(first, t).start()
            return carry2

        lax.fori_loop(0, TILES, load_body, 0)

        def layer_body(layer, carry2):
            cur = lax.rem(cycle * layers + layer, 2)
            nxt = 1 - cur
            for t in range(TILES):
                await_share(cur, t)
                share(cur, t).wait_send()

            def tile_body(t, carry3):
                @pl.when(jnp.logical_and(layer == 0, cycle == 0))
                def _():
                    for q in range(4):
                        a_copy(t, q).wait()
                state = hb[cur].reshape(COLS, 4 * VARS)
                for r in range(2):
                    mixed = jnp.dot(a_vm[t, 256 * r:256 * (r + 1), :], state, preferred_element_type=F32)
                    mt[256 * r:256 * (r + 1), :] = mixed.astype(BF16)
                sums = [None, None]
                for n in range(8):
                    for p in range(2):
                        lo = 256 * n
                        h = jnp.dot(mt[:, 128 * p:128 * (p + 1)], wp[layer, :, lo:lo + 256], preferred_element_type=F32)
                        z = h * (C1 + C2 * (h * h))
                        q_act = (h + h * jnp.tanh(z)).astype(BF16)
                        part = jnp.dot(q_act, up[layer, lo:lo + 256, :], preferred_element_type=F32)
                        sums[p] = part if sums[p] is None else sums[p] + part
                for p in range(2):
                    hf[t, :, 128 * p:128 * (p + 1)] = hf[t, :, 128 * p:128 * (p + 1)] + sums[p]

                @pl.when(layer < layers - 1)
                def _():
                    lane = pl.multiple_of(LANE * t, LANE)
                    for q in range(4):
                        hb[nxt, 4 * c + q, pl.ds(lane, LANE), :] = hf[t, LANE * q:LANE * (q + 1), :].astype(BF16)
                    share(nxt, t).start()

                @pl.when(layer == layers - 1)
                def _():
                    for q in range(4):
                        st[t, :, :, LANE * q:LANE * (q + 1)] = hf[t, LANE * q:LANE * (q + 1), :].T.reshape(4, VARS, LANE)
                    for q in range(4):
                        start(f_ship(t, q))
                return carry3

            return lax.fori_loop(0, TILES, tile_body, carry2)

        lax.fori_loop(0, layers, layer_body, 0)

        @pl.when(cycle > 0)
        def _():
            for t in range(TILES):
                for n in range(4):
                    sent(g_ship(t, n))

        def analysis_body(t, carry2):
            for s in range(4):
                await_bytes(xin.at[4 * s:4 * s + 4, :, pl.ds(pl.multiple_of(LANE * t, LANE), LANE)], frecv.at[t, s])

            def write(k, row, a, b):
                gst[t, k, row:row + 8, :] = a
                gst[t, k, row + 8:row + 16, :] = b
            analyse_tile(xin, t, idx_ref, obs_ref.at[cycle], prec_ref, rho_ref[0], ob, xa, mref, yo, gp, bm, zm, tm, wa, write)

            @pl.when(cycle < cycles - 1)
            def _():
                for n in range(4):
                    start(g_ship(t, n))

            @pl.when(cycle == cycles - 1)
            def _():
                for n in range(8):
                    start(o_ship(t, n))
            return carry2

        lax.fori_loop(0, TILES, analysis_body, 0)
        for t in range(TILES):
            for q in range(4):
                sent(f_ship(t, q))
        return carry

    lax.fori_loop(0, cycles, cycle_body, 0)
    for t in range(TILES):
        for n in range(8):
            sent(o_ship(t, n))
        for s in range(8):
            lo = BLK * s + LANE * t
            await_bytes(out_ref.at[:, :, lo:lo + LANE], orecv.at[t, s])


def run_cycles(ens_t, w_in, w_out_t, mix_op, obs_t, prec_t, obs_idx, rho):
    vm = pl.BlockSpec(memory_space=pltpu.VMEM)
    sm = pl.BlockSpec(memory_space=pltpu.SMEM)
    hbm = pl.BlockSpec(memory_space=pl.ANY)
    dma = pltpu.SemaphoreType.DMA
    layers, cycles = w_in.shape[0], obs_t.shape[0]
    return pl.pallas_call(
        functools.partial(cycle_kernel, layers, cycles),
        out_shape=jax.ShapeDtypeStruct((4, 32, COLS), F32),
        in_specs=[hbm, hbm, hbm, hbm, vm, vm, sm, sm],
        out_specs=hbm,
        scratch_shapes=[
            pltpu.VMEM((TILES, ROWS, COLS), BF16),
            pltpu.VMEM((2, 8, BLK, 4 * VARS), BF16),
            pltpu.VMEM((TILES, ROWS, 4 * VARS), F32),
            pltpu.VMEM((ROWS, 4 * VARS), BF16),
            pltpu.VMEM((TILES, 4, VARS, ROWS), F32),
            pltpu.VMEM((4, VARS, HALF), F32),
            pltpu.VMEM((K, VARS, BLK), F32),
            pltpu.VMEM((TILES, K, VARS, LANE), F32),
            pltpu.VMEM((2, layers, VARS, HID // 2), BF16),
            pltpu.VMEM((2, layers, VARS, HID // 2), BF16),
            pltpu.VMEM((layers, 2 * VARS, 2 * HID), BF16),
            pltpu.VMEM((layers, 2 * HID, 2 * VARS), BF16),
            pltpu.VMEM((64, LANE), F32),
            pltpu.VMEM((K * VARS, LANE), F32),
            pltpu.VMEM((VARS, LANE), F32),
            pltpu.VMEM((512, LANE), F32),
            pltpu.VMEM((512, LANE), F32),
            pltpu.VMEM((2, 256, LANE), F32),
            pltpu.VMEM((2, 256, LANE), F32),
            pltpu.VMEM((256, LANE), F32),
            pltpu.VMEM((256, LANE), F32),
            dma((TILES, 4)),
            dma((2,)),
            dma((2,)),
            dma((2,)),
            dma((2, 2)),
            dma((2, TILES)),
            dma((2, TILES)),
            dma((TILES, 4)),
            dma((TILES, 4)),
            dma((TILES, 4)),
            dma((TILES, 4)),
            dma((TILES, 8)),
            dma((TILES, 8)),
        ],
        compiler_params=pltpu.CompilerParams(collective_id=1, has_side_effects=True, vmem_limit_bytes=VMEM_LIMIT),
        name="cycle_all",
    )(ens_t, w_in, w_out_t, mix_op, obs_t, prec_t, obs_idx, rho)


def solution(mesh):
    def local_step(ens_local, mix_op, w_in, w_out, obs_val, obs_prec, obs_idx, inflation):
        out = run_cycles(
            jnp.transpose(ens_local, (0, 2, 1)), w_in, jnp.transpose(w_out, (0, 2, 1)), mix_op,
            jnp.transpose(obs_val, (0, 2, 1)), jnp.transpose(obs_prec, (1, 0)), obs_idx, inflation)
        return jnp.transpose(out, (0, 2, 1))

    member_spec = P(("case", "ens"), None, "model")
    col_axes = ("case", "ens", "model")
    in_specs = (member_spec, P(None, None), P(None, None, "model"), P(None, "model", None), P(None, col_axes, None), P(col_axes, None), P(None), P(None))
    return jax.shard_map(local_step, mesh=mesh, in_specs=in_specs, out_specs=member_spec, check_vma=False)
```

```python
import functools
import math

import jax
import jax.numpy as jnp
from jax import lax
from jax.experimental import pallas as pl
from jax.experimental.pallas import tpu as pltpu
from jax.sharding import PartitionSpec as P

MESH = pl.DeviceIdType.MESH
K = 16
COLS = 5120
VARS = 64
HID = 1024
BLK = 640
LANE = 128
TILES = 5
ROWS = 512
HALF = 2560
NS_STEPS = 12
VMEM_LIMIT = 64 * 1024 * 1024 - 64 * 1024
F32 = jnp.float32
BF16 = jnp.bfloat16
C0 = math.sqrt(2.0 / math.pi)
C1 = 2.0 * C0
C2 = 8.0 * 0.044715 * C0


def coords():
    e = lax.axis_index("ens")
    return e // 2, lax.axis_index("model"), e % 2


def dev(x, y, c):
    return {"model": y, "ens": 2 * x + c}


def greet():
    x, y, c = coords()
    barrier = pltpu.get_barrier_semaphore()
    for r in range(1, 8):
        dx, dy, dc = r // 4, (r // 2) % 2, r % 2
        pl.semaphore_signal(barrier, inc=1, device_id=dev((x + dx) % 2, (y + dy) % 2, (c + dc) % 2), device_id_type=MESH)
    pl.semaphore_wait(barrier, 7)


def await_bytes(ref, sem):
    pltpu.make_async_copy(ref, ref, sem).wait()


def bcast(ref, row):
    return ref[pl.ds(row, 8, stride=0), :]


def right_factor(ref):
    top = [(ref[16 * k:16 * k + 8, :], ref[16 * k + 8:16 * k + 16, :]) for k in range(8)]
    low = [(ref[pl.ds(8 + a, 8, stride=16), :], ref[16 * (8 + a) + 8:16 * (8 + a) + 16, :]) for a in range(8)]
    return top + low


def sym_row(i, k):
    return 16 * k + i if (i >= 8 and k < 8) else 16 * i + k


def sym_product(left, right, emit):
    cols = right_factor(right)
    for i in range(16):
        lo = hi = None
        for k in range(16):
            s = bcast(left, sym_row(i, k))
            if i < 8:
                lo = s * cols[k][0] if lo is None else lo + s * cols[k][0]
            hi = s * cols[k][1] if hi is None else hi + s * cols[k][1]
        emit(i, lo, hi)


def analyse_tile(xin, t, idx_ref, yo_ref, ri_ref, rho, ob, xa, mref, yo, gp, bm, zm, tm, wa, write):
    lanes = pl.ds(pl.multiple_of(LANE * t, LANE), LANE)
    sub = lax.broadcasted_iota(jnp.int32, (8, LANE), 0)
    for v in range(8):
        rows = slice(8 * v, 8 * v + 8)
        vals = [xin[t, k, rows, :] for k in range(K)]
        total = vals[0]
        for k in range(1, K):
            total = total + vals[k]
        mean = total * (1.0 / K)
        mref[rows, :] = mean
        for k in range(K):
            xa[VARS * k + 8 * v:VARS * k + 8 * v + 8, :] = vals[k] - mean

    ob[0:32, :] = yo_ref[:, lanes]
    ob[32:64, :] = ri_ref[:, lanes]
    for p in range(32):
        col = idx_ref[p]
        y_lo = xa[pl.ds(col, 8, stride=VARS), :]
        y_hi = xa[pl.ds(col + 8 * VARS, 8, stride=VARS), :]
        prec = bcast(ob, 32 + p)
        yo[16 * p:16 * p + 8, :] = y_lo
        yo[16 * p + 8:16 * p + 16, :] = y_hi
        gp[16 * p:16 * p + 8, :] = y_lo * prec
        gp[16 * p + 8:16 * p + 16, :] = y_hi * prec
    g_lo = jnp.zeros((8, LANE), F32)
    g_hi = jnp.zeros((8, LANE), F32)
    for p in range(32):
        inno = bcast(ob, p) - bcast(mref, idx_ref[p])
        g_lo = g_lo + gp[16 * p:16 * p + 8, :] * inno
        g_hi = g_hi + gp[16 * p + 8:16 * p + 16, :] * inno
    diag = (K - 1) / rho
    trace = jnp.zeros((8, LANE), F32)
    for half in range(2):
        acc = [None] * 8
        acc2 = [None] * 8
        for p in range(32):
            y_lo = yo[16 * p:16 * p + 8, :]
            y_hi = yo[16 * p + 8:16 * p + 16, :]
            for r in range(8):
                s = bcast(gp, 16 * p + 8 * half + r)
                if half == 0:
                    acc[r] = s * y_lo if acc[r] is None else acc[r] + s * y_lo
                acc2[r] = s * y_hi if acc2[r] is None else acc2[r] + s * y_hi
        for r in range(8):
            i = 8 * half + r
            on = sub == r
            if half == 0:
                d = jnp.where(on, acc[r] + diag, acc[r])
                trace = trace + jnp.where(on, d, 0.0)
                bm[0, 16 * i:16 * i + 8, :] = d
                bm[0, 16 * i + 8:16 * i + 16, :] = acc2[r]
            else:
                d = jnp.where(on, acc2[r] + diag, acc2[r])
                trace = trace + jnp.where(on, d, 0.0)
                bm[0, 16 * i + 8:16 * i + 16, :] = d
    trace = jnp.broadcast_to(jnp.sum(trace, axis=0, keepdims=True), (8, LANE))
    inv = 1.0 / trace

    def slots(i):
        out = [(16 * i + 8, i >= 8)]
        if i < 8:
            out.append((16 * i, True))
        return out

    for i in range(16):
        for row, has_diag in slots(i):
            b = bm[0, row:row + 8, :] * inv
            bm[0, row:row + 8, :] = b
            z = b * -0.5
            if has_diag:
                z = jnp.where(sub == i % 8, z + 1.5, z)
            tm[row:row + 8, :] = z
            zm[0, row:row + 8, :] = z

    def emit_to(ref):
        def emit(i, lo, hi):
            if lo is not None:
                ref[16 * i:16 * i + 8, :] = lo
            ref[16 * i + 8:16 * i + 16, :] = hi
        return emit

    def emit_t(i, lo, hi):
        hi = hi * -0.5
        if lo is not None:
            lo = lo * -0.5
            tm[16 * i:16 * i + 8, :] = jnp.where(sub == i % 8, lo + 1.5, lo)
        else:
            hi = jnp.where(sub == i % 8, hi + 1.5, hi)
        tm[16 * i + 8:16 * i + 16, :] = hi

    def ns_step(step, carry):
        cur = lax.rem(step, 2)
        nxt = 1 - cur
        b_cur, b_nxt = bm.at[cur], bm.at[nxt]
        z_cur, z_nxt = zm.at[cur], zm.at[nxt]
        sym_product(b_cur, tm, emit_to(b_nxt))
        sym_product(z_cur, b_nxt, emit_t)
        sym_product(tm, z_cur, emit_to(z_nxt))
        return carry

    lax.fori_loop(0, NS_STEPS - 1, ns_step, 0)
    last = (NS_STEPS - 1) % 2
    z_fin = zm.at[last]

    root = 1.0 / jnp.sqrt(trace)
    cols = [(lo * root, hi * root) for lo, hi in right_factor(z_fin)]

    def sym_apply(lo, hi):
        gp[0:8, :] = lo
        gp[8:16, :] = hi
        a = b = None
        for k in range(16):
            s = bcast(gp, k)
            a = s * cols[k][0] if a is None else a + s * cols[k][0]
            b = s * cols[k][1] if b is None else b + s * cols[k][1]
        return a, b

    h_lo, h_hi = sym_apply(g_lo, g_hi)
    w_lo, w_hi = sym_apply(h_lo, h_hi)
    gp[0:8, :] = w_lo
    gp[8:16, :] = w_hi
    scale = math.sqrt(K - 1)
    for i in range(16):
        w = bcast(gp, i)
        wa[16 * i:16 * i + 8, :] = cols[i][0] * scale + w
        wa[16 * i + 8:16 * i + 16, :] = cols[i][1] * scale + w

    for v in range(0, 8, 2):
        xs = [(xa[VARS * i + 8 * v:VARS * i + 8 * v + 8, :], xa[VARS * i + 8 * v + 8:VARS * i + 8 * v + 16, :]) for i in range(K)]
        for k in range(K):
            a = mref[8 * v:8 * v + 8, :]
            b = mref[8 * v + 8:8 * v + 16, :]
            for i in range(K):
                s = bcast(wa, 16 * i + k)
                a = a + s * xs[i][0]
                b = b + s * xs[i][1]
            write(k, 8 * v, a, b)


def either(flag, yes, no):
    if flag is True:
        yes()
    elif flag is False:
        no()
    else:
        pl.when(flag)(yes)
        pl.when(jnp.logical_not(flag))(no)


def cycle_kernel(layers, cycles, ens_ref, win_ref, wout_ref, a_ref, obs_ref, prec_ref, idx_ref, rho_ref, out_ref,
                 a_vm, hb, hf, mt, st, ht, xin, gst, wr, ur, wp, up,
                 ob, xa, mref, yo, gp, bm, zm, tm, wa,
                 a_sem, isend, irecv, wsend, wrecv, xsend, xrecv, fsend, frecv, gsend, grecv, osend, orecv):
    x, y, c = coords()
    partner = dev(x, y, 1 - c)
    greet()

    def init_piece(h, t, q):
        src = ens_ref.at[:, :, pl.ds(HALF * h + BLK * q + LANE * t, LANE)]
        dst = ht.at[t, q, :, pl.ds(pl.multiple_of(32 * y, 32), 32), :]
        is_self = jnp.logical_and(c == y, c == h)
        rsem = irecv.at[t, q, y]

        def local():
            return pltpu.make_async_copy(src, dst, rsem)

        def remote():
            return pltpu.make_async_remote_copy(src, dst, isend.at[h, t, q], rsem, device_id=dev(x, c, h), device_id_type=MESH)
        return is_self, local, remote

    weights = ((win_ref, wr), (wout_ref, ur))

    def weight_local(n):
        src, dst = weights[n]
        return pltpu.make_async_copy(src, dst.at[y], wrecv.at[n, 1])

    @pl.when(c == y)
    def _():
        for n, (src, dst) in enumerate(weights):
            pltpu.make_async_remote_copy(src, dst.at[y], wsend.at[n], wrecv.at[n, 0], device_id=dev(x, 1 - y, c), device_id_type=MESH).start()

    for n in range(2):
        weight_local(n).start()
    for t in range(TILES):
        for q in range(4):
            for h in range(2):
                is_self, local, remote = init_piece(h, t, q)
                either(is_self, lambda: local().start(), lambda: remote().start())

    def a_copy(t, q):
        row = pl.multiple_of((4 * c + q) * BLK + LANE * t, LANE)
        return pltpu.make_async_copy(a_ref.at[pl.ds(row, LANE), :], a_vm.at[t, pl.ds(LANE * q, LANE), :], a_sem.at[t, q])

    for t in range(TILES):
        for q in range(4):
            a_copy(t, q).start()

    for n in range(2):
        weight_local(n).wait()
    for n, (src, dst) in enumerate(weights):
        piece = dst.at[1 - y]
        await_bytes(piece, wrecv.at[n, 0])

        @pl.when(c != y)
        def _():
            pltpu.make_async_remote_copy(piece, piece, wsend.at[n], wrecv.at[n, 0], device_id=partner, device_id_type=MESH).start()
    for n, (src, dst) in enumerate(weights):
        await_bytes(dst.at[1 - y], wsend.at[n])
    for layer in range(layers):
        for part in range(2):
            for p in range(2):
                lo = HID * p + 512 * part
                wv = (wr[part, layer].astype(F32) * 0.5).astype(BF16)
                wz = jnp.zeros_like(wv)
                wp[layer, :, lo:lo + 512] = jnp.concatenate([wv, wz] if p == 0 else [wz, wv], axis=0)
                uv = ur[part, layer].astype(F32)
                uz = jnp.zeros_like(uv)
                up[layer, lo:lo + 512, :] = jnp.concatenate([uv, uz] if p == 0 else [uz, uv], axis=0).T.astype(BF16)

    def share(buf, t):
        lane = pl.multiple_of(LANE * t, LANE)
        piece = hb.at[buf, pl.ds(4 * c, 4), pl.ds(lane, LANE), :]
        return pltpu.make_async_remote_copy(piece, piece, xsend.at[buf, t], xrecv.at[buf, t], device_id=partner, device_id_type=MESH)

    def await_share(buf, t):
        lane = pl.multiple_of(LANE * t, LANE)
        await_bytes(hb.at[buf, pl.ds(4 * (1 - c), 4), pl.ds(lane, LANE), :], xrecv.at[buf, t])

    mine = 4 * (2 * x + y)

    def f_ship(t, q):
        c2, y2 = q // 2, q % 2
        src = st.at[t, q]
        dst = xin.at[t, pl.ds(mine, 4)]
        is_self = jnp.logical_and(x == c, jnp.logical_and(c == c2, y == y2))
        rsem = frecv.at[t, 2 * x + y]

        def local():
            return pltpu.make_async_copy(src, dst, rsem)

        def remote():
            return pltpu.make_async_remote_copy(src, dst, fsend.at[t, q], rsem, device_id=dev(c, y2, c2), device_id_type=MESH)
        return is_self, local, remote

    block = 4 * x + 2 * c + y
    back = [(1, 1), (1, 0), (0, 1), (0, 0)]

    def g_ship(t, n):
        dx, dy = back[n]
        x2, y2 = (x + dx) % 2, (y + dy) % 2
        src = gst.at[t, pl.ds(4 * (2 * x2 + y2), 4), :, :]
        dst = ht.at[t, 2 * c + y]
        rsem = grecv.at[t, 2 * c + y]
        is_self = (x == c) if n == 3 else False

        def local():
            return pltpu.make_async_copy(src, dst, rsem)

        def remote():
            return pltpu.make_async_remote_copy(src, dst, gsend.at[t, n], rsem, device_id=dev(x2, y2, x), device_id_type=MESH)
        return is_self, local, remote

    def o_ship(t, n):
        r = 7 - n
        x2, y2, c2 = (x + r // 4) % 2, (y + (r // 2) % 2) % 2, (c + r % 2) % 2
        lane = pl.multiple_of(block * BLK + LANE * t, LANE)
        src = gst.at[t, pl.ds(4 * (2 * x2 + c2), 4), pl.ds(pl.multiple_of(32 * y2, 32), 32), :]
        dst = out_ref.at[:, :, pl.ds(lane, LANE)]
        rsem = orecv.at[t, block]

        def local():
            return pltpu.make_async_copy(src, dst, rsem)

        def remote():
            return pltpu.make_async_remote_copy(src, dst, osend.at[t, n], rsem, device_id=dev(x2, y2, c2), device_id_type=MESH)
        return r == 0, local, remote

    def start(ship):
        is_self, local, remote = ship
        either(is_self, lambda: local().start(), lambda: remote().start())

    def sent(ship):
        is_self, local, remote = ship
        either(is_self, lambda: None, lambda: remote().wait_send())

    def cycle_body(cycle, carry):
        first = lax.rem(cycle * layers, 2)

        def load_body(t, carry2):
            @pl.when(cycle == 0)
            def _():
                for q in range(4):
                    for s in range(2):
                        await_bytes(ht.at[t, q, :, 32 * s:32 * s + 32, :], irecv.at[t, q, s])

            @pl.when(cycle > 0)
            def _():
                for s in range(4):
                    await_bytes(ht.at[t, s], grecv.at[t, s])
            lane = pl.multiple_of(LANE * t, LANE)
            for q in range(4):
                part = ht[t, q].reshape(4 * VARS, LANE).T
                hf[t, LANE * q:LANE * (q + 1), :] = part
                hb[first, 4 * c + q, pl.ds(lane, LANE), :] = part.astype(BF16)
            share(first, t).start()
            return carry2

        lax.fori_loop(0, TILES, load_body, 0)

        @pl.when(cycle == 0)
        def _():
            for t in range(TILES):
                for q in range(4):
                    for h in range(2):
                        sent(init_piece(h, t, q))

        def layer_body(layer, carry2):
            cur = lax.rem(cycle * layers + layer, 2)
            nxt = 1 - cur
            late = TILES - 1
            for t in range(late):
                await_share(cur, t)

            def await_rows(t):
                @pl.when(jnp.logical_and(layer == 0, cycle == 0))
                def _():
                    for q in range(4):
                        a_copy(t, q).wait()

            def first_mix():
                def lates(r, core):
                    out = None
                    for j in range(4):
                        lo = pl.multiple_of((4 * core + j) * BLK + LANE * late, LANE)
                        part = jnp.dot(a_vm[0, 256 * r:256 * (r + 1), pl.ds(lo, LANE)], hb[cur, 4 * core + j, LANE * late:, :], preferred_element_type=F32)
                        out = part if out is None else out + part
                    return out
                early = []
                for r in range(2):
                    acc = None
                    for b in range(8):
                        part = jnp.dot(a_vm[0, 256 * r:256 * (r + 1), BLK * b:BLK * b + LANE * late], hb[cur, b, :LANE * late, :], preferred_element_type=F32)
                        acc = part if acc is None else acc + part
                    early.append(acc + lates(r, c))
                await_share(cur, late)
                for r in range(2):
                    mt[256 * r:256 * (r + 1), :] = (early[r] + lates(r, 1 - c)).astype(BF16)

            def full_mix(t):
                state = hb[cur].reshape(COLS, 4 * VARS)
                for r in range(2):
                    mixed = jnp.dot(a_vm[t, 256 * r:256 * (r + 1), :], state, preferred_element_type=F32)
                    mt[256 * r:256 * (r + 1), :] = mixed.astype(BF16)

            def finish(t):
                sums = [None, None]
                for n in range(8):
                    for p in range(2):
                        lo = 256 * n
                        h = jnp.dot(mt[:, 128 * p:128 * (p + 1)], wp[layer, :, lo:lo + 256], preferred_element_type=F32)
                        z = h * (C1 + C2 * (h * h))
                        q_act = (h + h * jnp.tanh(z)).astype(BF16)
                        part = jnp.dot(q_act, up[layer, lo:lo + 256, :], preferred_element_type=F32)
                        sums[p] = part if sums[p] is None else sums[p] + part
                for p in range(2):
                    hf[t, :, 128 * p:128 * (p + 1)] = hf[t, :, 128 * p:128 * (p + 1)] + sums[p]

                @pl.when(layer < layers - 1)
                def _():
                    lane = pl.multiple_of(LANE * t, LANE)
                    for q in range(4):
                        hb[nxt, 4 * c + q, pl.ds(lane, LANE), :] = hf[t, LANE * q:LANE * (q + 1), :].astype(BF16)
                    share(nxt, t).start()

                @pl.when(layer == layers - 1)
                def _():
                    for q in range(4):
                        st[t, q] = hf[t, LANE * q:LANE * (q + 1), :].T.reshape(4, VARS, LANE)
                    for q in range(4):
                        start(f_ship(t, q))

            def tile_body(t, carry3):
                await_rows(t)
                full_mix(t)
                finish(t)
                return carry3

            await_rows(0)
            first_mix()
            finish(0)
            for t in range(TILES):
                share(cur, t).wait_send()
            return lax.fori_loop(1, TILES, tile_body, carry2)

        lax.fori_loop(0, layers, layer_body, 0)

        @pl.when(cycle > 0)
        def _():
            for t in range(TILES):
                for n in range(4):
                    sent(g_ship(t, n))

        def analysis_body(t, carry2):
            for s in range(4):
                await_bytes(xin.at[t, 4 * s:4 * s + 4], frecv.at[t, s])

            def write(k, row, a, b):
                gst[t, k, row:row + 8, :] = a
                gst[t, k, row + 8:row + 16, :] = b
            analyse_tile(xin, t, idx_ref, obs_ref.at[cycle], prec_ref, rho_ref[0], ob, xa, mref, yo, gp, bm, zm, tm, wa, write)

            @pl.when(cycle < cycles - 1)
            def _():
                for n in range(4):
                    start(g_ship(t, n))

            @pl.when(cycle == cycles - 1)
            def _():
                for n in range(8):
                    start(o_ship(t, n))
            return carry2

        lax.fori_loop(0, TILES, analysis_body, 0)
        for t in range(TILES):
            for q in range(4):
                sent(f_ship(t, q))
        return carry

    lax.fori_loop(0, cycles, cycle_body, 0)
    for t in range(TILES):
        for n in range(8):
            sent(o_ship(t, n))
        for s in range(8):
            lo = BLK * s + LANE * t
            await_bytes(out_ref.at[:, :, lo:lo + LANE], orecv.at[t, s])


def run_cycles(ens_t, w_in, w_out_t, mix_op, obs_t, prec_t, obs_idx, rho):
    vm = pl.BlockSpec(memory_space=pltpu.VMEM)
    sm = pl.BlockSpec(memory_space=pltpu.SMEM)
    hbm = pl.BlockSpec(memory_space=pl.ANY)
    dma = pltpu.SemaphoreType.DMA
    layers, cycles = w_in.shape[0], obs_t.shape[0]
    return pl.pallas_call(
        functools.partial(cycle_kernel, layers, cycles),
        out_shape=jax.ShapeDtypeStruct((4, 32, COLS), F32),
        in_specs=[hbm, hbm, hbm, hbm, vm, vm, sm, sm],
        out_specs=hbm,
        scratch_shapes=[
            pltpu.VMEM((TILES, ROWS, COLS), BF16),
            pltpu.VMEM((2, 8, BLK, 4 * VARS), BF16),
            pltpu.VMEM((TILES, ROWS, 4 * VARS), F32),
            pltpu.VMEM((ROWS, 4 * VARS), BF16),
            pltpu.VMEM((TILES, 4, 4, VARS, LANE), F32),
            pltpu.VMEM((TILES, 4, 4, VARS, LANE), F32),
            pltpu.VMEM((TILES, K, VARS, LANE), F32),
            pltpu.VMEM((TILES, K, VARS, LANE), F32),
            pltpu.VMEM((2, layers, VARS, HID // 2), BF16),
            pltpu.VMEM((2, layers, VARS, HID // 2), BF16),
            pltpu.VMEM((layers, 2 * VARS, 2 * HID), BF16),
            pltpu.VMEM((layers, 2 * HID, 2 * VARS), BF16),
            pltpu.VMEM((64, LANE), F32),
            pltpu.VMEM((K * VARS, LANE), F32),
            pltpu.VMEM((VARS, LANE), F32),
            pltpu.VMEM((512, LANE), F32),
            pltpu.VMEM((512, LANE), F32),
            pltpu.VMEM((2, 256, LANE), F32),
            pltpu.VMEM((2, 256, LANE), F32),
            pltpu.VMEM((256, LANE), F32),
            pltpu.VMEM((256, LANE), F32),
            dma((TILES, 4)),
            dma((2, TILES, 4)),
            dma((TILES, 4, 2)),
            dma((2,)),
            dma((2, 2)),
            dma((2, TILES)),
            dma((2, TILES)),
            dma((TILES, 4)),
            dma((TILES, 4)),
            dma((TILES, 4)),
            dma((TILES, 4)),
            dma((TILES, 8)),
            dma((TILES, 8)),
        ],
        compiler_params=pltpu.CompilerParams(collective_id=1, has_side_effects=True, vmem_limit_bytes=VMEM_LIMIT),
        name="cycle_all",
    )(ens_t, w_in, w_out_t, mix_op, obs_t, prec_t, obs_idx, rho)


def solution(mesh):
    def local_step(ens_local, mix_op, w_in, w_out, obs_val, obs_prec, obs_idx, inflation):
        out = run_cycles(
            jnp.transpose(ens_local, (0, 2, 1)), w_in, jnp.transpose(w_out, (0, 2, 1)), mix_op,
            jnp.transpose(obs_val, (0, 2, 1)), jnp.transpose(obs_prec, (1, 0)), obs_idx, inflation)
        return jnp.transpose(out, (0, 2, 1))

    member_spec = P(("case", "ens"), None, "model")
    col_axes = ("case", "ens", "model")
    in_specs = (member_spec, P(None, None), P(None, None, "model"), P(None, "model", None), P(None, col_axes, None), P(col_axes, None), P(None), P(None))
    return jax.shard_map(local_step, mesh=mesh, in_specs=in_specs, out_specs=member_spec, check_vma=False)
```

```python
import functools
import math

import jax
import jax.numpy as jnp
from jax import lax
from jax.experimental import pallas as pl
from jax.experimental.pallas import tpu as pltpu
from jax.sharding import PartitionSpec as P

MESH = pl.DeviceIdType.MESH
K = 16
COLS = 5120
VARS = 64
HID = 1024
BLK = 640
LANE = 128
TILES = 5
ROWS = 512
HALF = 2560
CHUNK = 1024
NS_STEPS = 12
VMEM_LIMIT = 64 * 1024 * 1024 - 64 * 1024
F32 = jnp.float32
BF16 = jnp.bfloat16
C0 = math.sqrt(2.0 / math.pi)
C1 = 2.0 * C0
C2 = 8.0 * 0.044715 * C0


def coords():
    e = lax.axis_index("ens")
    return e // 2, lax.axis_index("model"), e % 2


def dev(x, y, c):
    return {"model": y, "ens": 2 * x + c}


def greet():
    x, y, c = coords()
    barrier = pltpu.get_barrier_semaphore()
    for r in range(1, 8):
        dx, dy, dc = r // 4, (r // 2) % 2, r % 2
        pl.semaphore_signal(barrier, inc=1, device_id=dev((x + dx) % 2, (y + dy) % 2, (c + dc) % 2), device_id_type=MESH)
    pl.semaphore_wait(barrier, 7)


def await_bytes(ref, sem):
    pltpu.make_async_copy(ref, ref, sem).wait()


def bcast(ref, row):
    return ref[pl.ds(row, 8, stride=0), :]


def right_factor(ref):
    top = [(ref[16 * k:16 * k + 8, :], ref[16 * k + 8:16 * k + 16, :]) for k in range(8)]
    low = [(ref[pl.ds(8 + a, 8, stride=16), :], ref[16 * (8 + a) + 8:16 * (8 + a) + 16, :]) for a in range(8)]
    return top + low


def sym_row(i, k):
    return 16 * k + i if (i >= 8 and k < 8) else 16 * i + k


def sym_product(left, right, emit):
    cols = right_factor(right)
    for i in range(16):
        lo = hi = None
        for k in range(16):
            s = bcast(left, sym_row(i, k))
            if i < 8:
                lo = s * cols[k][0] if lo is None else lo + s * cols[k][0]
            hi = s * cols[k][1] if hi is None else hi + s * cols[k][1]
        emit(i, lo, hi)


def analyse_tile(xin, t, idx_ref, yo_ref, ri_ref, rho, ob, xa, mref, yo, gp, bm, zm, tm, wa, write):
    lanes = pl.ds(pl.multiple_of(LANE * t, LANE), LANE)
    sub = lax.broadcasted_iota(jnp.int32, (8, LANE), 0)
    for v in range(8):
        rows = slice(8 * v, 8 * v + 8)
        vals = [xin[t, k, rows, :] for k in range(K)]
        total = vals[0]
        for k in range(1, K):
            total = total + vals[k]
        mean = total * (1.0 / K)
        mref[rows, :] = mean
        for k in range(K):
            xa[VARS * k + 8 * v:VARS * k + 8 * v + 8, :] = vals[k] - mean

    ob[0:32, :] = yo_ref[:, lanes]
    ob[32:64, :] = ri_ref[:, lanes]
    for p in range(32):
        col = idx_ref[p]
        y_lo = xa[pl.ds(col, 8, stride=VARS), :]
        y_hi = xa[pl.ds(col + 8 * VARS, 8, stride=VARS), :]
        prec = bcast(ob, 32 + p)
        yo[16 * p:16 * p + 8, :] = y_lo
        yo[16 * p + 8:16 * p + 16, :] = y_hi
        gp[16 * p:16 * p + 8, :] = y_lo * prec
        gp[16 * p + 8:16 * p + 16, :] = y_hi * prec
    g_lo = jnp.zeros((8, LANE), F32)
    g_hi = jnp.zeros((8, LANE), F32)
    for p in range(32):
        inno = bcast(ob, p) - bcast(mref, idx_ref[p])
        g_lo = g_lo + gp[16 * p:16 * p + 8, :] * inno
        g_hi = g_hi + gp[16 * p + 8:16 * p + 16, :] * inno
    diag = (K - 1) / rho
    trace = jnp.zeros((8, LANE), F32)
    for half in range(2):
        acc = [None] * 8
        acc2 = [None] * 8
        for p in range(32):
            y_lo = yo[16 * p:16 * p + 8, :]
            y_hi = yo[16 * p + 8:16 * p + 16, :]
            for r in range(8):
                s = bcast(gp, 16 * p + 8 * half + r)
                if half == 0:
                    acc[r] = s * y_lo if acc[r] is None else acc[r] + s * y_lo
                acc2[r] = s * y_hi if acc2[r] is None else acc2[r] + s * y_hi
        for r in range(8):
            i = 8 * half + r
            on = sub == r
            if half == 0:
                d = jnp.where(on, acc[r] + diag, acc[r])
                trace = trace + jnp.where(on, d, 0.0)
                bm[0, 16 * i:16 * i + 8, :] = d
                bm[0, 16 * i + 8:16 * i + 16, :] = acc2[r]
            else:
                d = jnp.where(on, acc2[r] + diag, acc2[r])
                trace = trace + jnp.where(on, d, 0.0)
                bm[0, 16 * i + 8:16 * i + 16, :] = d
    trace = jnp.broadcast_to(jnp.sum(trace, axis=0, keepdims=True), (8, LANE))
    inv = 1.0 / trace

    def slots(i):
        out = [(16 * i + 8, i >= 8)]
        if i < 8:
            out.append((16 * i, True))
        return out

    for i in range(16):
        for row, has_diag in slots(i):
            b = bm[0, row:row + 8, :] * inv
            bm[0, row:row + 8, :] = b
            z = b * -0.5
            if has_diag:
                z = jnp.where(sub == i % 8, z + 1.5, z)
            tm[row:row + 8, :] = z
            zm[0, row:row + 8, :] = z

    def emit_to(ref):
        def emit(i, lo, hi):
            if lo is not None:
                ref[16 * i:16 * i + 8, :] = lo
            ref[16 * i + 8:16 * i + 16, :] = hi
        return emit

    def emit_t(i, lo, hi):
        hi = hi * -0.5
        if lo is not None:
            lo = lo * -0.5
            tm[16 * i:16 * i + 8, :] = jnp.where(sub == i % 8, lo + 1.5, lo)
        else:
            hi = jnp.where(sub == i % 8, hi + 1.5, hi)
        tm[16 * i + 8:16 * i + 16, :] = hi

    def ns_step(step, carry):
        cur = lax.rem(step, 2)
        nxt = 1 - cur
        b_cur, b_nxt = bm.at[cur], bm.at[nxt]
        z_cur, z_nxt = zm.at[cur], zm.at[nxt]
        sym_product(b_cur, tm, emit_to(b_nxt))
        sym_product(z_cur, b_nxt, emit_t)
        sym_product(tm, z_cur, emit_to(z_nxt))
        return carry

    lax.fori_loop(0, NS_STEPS - 1, ns_step, 0)
    last = (NS_STEPS - 1) % 2
    z_fin = zm.at[last]

    root = 1.0 / jnp.sqrt(trace)
    cols = [(lo * root, hi * root) for lo, hi in right_factor(z_fin)]

    def sym_apply(lo, hi):
        gp[0:8, :] = lo
        gp[8:16, :] = hi
        a = b = None
        for k in range(16):
            s = bcast(gp, k)
            a = s * cols[k][0] if a is None else a + s * cols[k][0]
            b = s * cols[k][1] if b is None else b + s * cols[k][1]
        return a, b

    h_lo, h_hi = sym_apply(g_lo, g_hi)
    w_lo, w_hi = sym_apply(h_lo, h_hi)
    gp[0:8, :] = w_lo
    gp[8:16, :] = w_hi
    scale = math.sqrt(K - 1)
    for i in range(16):
        w = bcast(gp, i)
        wa[16 * i:16 * i + 8, :] = cols[i][0] * scale + w
        wa[16 * i + 8:16 * i + 16, :] = cols[i][1] * scale + w

    for v in range(0, 8, 2):
        xs = [(xa[VARS * i + 8 * v:VARS * i + 8 * v + 8, :], xa[VARS * i + 8 * v + 8:VARS * i + 8 * v + 16, :]) for i in range(K)]
        for k in range(K):
            a = mref[8 * v:8 * v + 8, :]
            b = mref[8 * v + 8:8 * v + 16, :]
            for i in range(K):
                s = bcast(wa, 16 * i + k)
                a = a + s * xs[i][0]
                b = b + s * xs[i][1]
            write(k, 8 * v, a, b)


def either(flag, yes, no):
    if flag is True:
        yes()
    elif flag is False:
        no()
    else:
        pl.when(flag)(yes)
        pl.when(jnp.logical_not(flag))(no)


def cycle_kernel(layers, cycles, ens_ref, win_ref, wout_ref, a_ref, obs_ref, prec_ref, idx_ref, rho_ref, out_ref,
                 a_vm, hb, hf, mt, macc, st, ht, xin, gst, wr, ur, wp, up,
                 ob, xa, mref, yo, gp, bm, zm, tm, wa,
                 a_sem, isend, irecv, wsend, wrecv, xsend, xrecv, fsend, frecv, gsend, grecv, osend, orecv):
    x, y, c = coords()
    partner = dev(x, y, 1 - c)
    greet()

    def init_piece(h, t, q):
        src = ens_ref.at[:, :, pl.ds(HALF * h + BLK * q + LANE * t, LANE)]
        dst = ht.at[t, q, :, pl.ds(pl.multiple_of(32 * y, 32), 32), :]
        is_self = jnp.logical_and(c == y, c == h)
        rsem = irecv.at[t, q, y]

        def local():
            return pltpu.make_async_copy(src, dst, rsem)

        def remote():
            return pltpu.make_async_remote_copy(src, dst, isend.at[h, t, q], rsem, device_id=dev(x, c, h), device_id_type=MESH)
        return is_self, local, remote

    weights = ((win_ref, wr), (wout_ref, ur))

    def weight_local(n):
        src, dst = weights[n]
        return pltpu.make_async_copy(src, dst.at[y], wrecv.at[n, 1])

    @pl.when(c == y)
    def _():
        for n, (src, dst) in enumerate(weights):
            pltpu.make_async_remote_copy(src, dst.at[y], wsend.at[n], wrecv.at[n, 0], device_id=dev(x, 1 - y, c), device_id_type=MESH).start()

    for n in range(2):
        weight_local(n).start()
    for t in range(TILES):
        for q in range(4):
            for h in range(2):
                is_self, local, remote = init_piece(h, t, q)
                either(is_self, lambda: local().start(), lambda: remote().start())

    def a_copy(t, q):
        src = a_ref.at[pl.ds(pl.multiple_of(HALF * c, HALF), HALF), pl.ds(pl.multiple_of(BLK * q + LANE * t, LANE), LANE)]
        return pltpu.make_async_copy(src, a_vm.at[:, pl.ds(pl.multiple_of(CHUNK * t + LANE * q, LANE), LANE)], a_sem.at[t, q])

    for t in range(TILES):
        for q in range(8):
            a_copy(t, q).start()

    def a_rows(t, r, lo, size):
        cols = pl.ds(lo, size)
        return jnp.concatenate([a_vm[pl.ds(pl.multiple_of(BLK * q + LANE * t, LANE), LANE), cols] for q in (2 * r, 2 * r + 1)], axis=0)

    for n in range(2):
        weight_local(n).wait()
    for n, (src, dst) in enumerate(weights):
        piece = dst.at[1 - y]
        await_bytes(piece, wrecv.at[n, 0])

        @pl.when(c != y)
        def _():
            pltpu.make_async_remote_copy(piece, piece, wsend.at[n], wrecv.at[n, 0], device_id=partner, device_id_type=MESH).start()
    for n, (src, dst) in enumerate(weights):
        await_bytes(dst.at[1 - y], wsend.at[n])
    for layer in range(layers):
        for part in range(2):
            for p in range(2):
                lo = HID * p + 512 * part
                wv = (wr[part, layer].astype(F32) * 0.5).astype(BF16)
                wz = jnp.zeros_like(wv)
                wp[layer, :, lo:lo + 512] = jnp.concatenate([wv, wz] if p == 0 else [wz, wv], axis=0)
                uv = ur[part, layer].astype(F32)
                uz = jnp.zeros_like(uv)
                up[layer, lo:lo + 512, :] = jnp.concatenate([uv, uz] if p == 0 else [uz, uv], axis=0).T.astype(BF16)

    def share(buf, t):
        piece = hb.at[buf, t, pl.ds(4 * c, 4)]
        return pltpu.make_async_remote_copy(piece, piece, xsend.at[buf, t], xrecv.at[buf, t], device_id=partner, device_id_type=MESH)

    def await_share(buf, t):
        await_bytes(hb.at[buf, t, pl.ds(4 * (1 - c), 4)], xrecv.at[buf, t])

    mine = 4 * (2 * x + y)

    def f_ship(t, q):
        c2, y2 = q // 2, q % 2
        src = st.at[t, q]
        dst = xin.at[t, pl.ds(mine, 4)]
        is_self = jnp.logical_and(x == c, jnp.logical_and(c == c2, y == y2))
        rsem = frecv.at[t, 2 * x + y]

        def local():
            return pltpu.make_async_copy(src, dst, rsem)

        def remote():
            return pltpu.make_async_remote_copy(src, dst, fsend.at[t, q], rsem, device_id=dev(c, y2, c2), device_id_type=MESH)
        return is_self, local, remote

    block = 4 * x + 2 * c + y
    back = [(1, 1), (1, 0), (0, 1), (0, 0)]

    def g_ship(t, n):
        dx, dy = back[n]
        x2, y2 = (x + dx) % 2, (y + dy) % 2
        src = gst.at[t, pl.ds(4 * (2 * x2 + y2), 4), :, :]
        dst = ht.at[t, 2 * c + y]
        rsem = grecv.at[t, 2 * c + y]
        is_self = (x == c) if n == 3 else False

        def local():
            return pltpu.make_async_copy(src, dst, rsem)

        def remote():
            return pltpu.make_async_remote_copy(src, dst, gsend.at[t, n], rsem, device_id=dev(x2, y2, x), device_id_type=MESH)
        return is_self, local, remote

    def o_ship(t, n):
        r = 7 - n
        x2, y2, c2 = (x + r // 4) % 2, (y + (r // 2) % 2) % 2, (c + r % 2) % 2
        lane = pl.multiple_of(block * BLK + LANE * t, LANE)
        src = gst.at[t, pl.ds(4 * (2 * x2 + c2), 4), pl.ds(pl.multiple_of(32 * y2, 32), 32), :]
        dst = out_ref.at[:, :, pl.ds(lane, LANE)]
        rsem = orecv.at[t, block]

        def local():
            return pltpu.make_async_copy(src, dst, rsem)

        def remote():
            return pltpu.make_async_remote_copy(src, dst, osend.at[t, n], rsem, device_id=dev(x2, y2, c2), device_id_type=MESH)
        return r == 0, local, remote

    def start(ship):
        is_self, local, remote = ship
        either(is_self, lambda: local().start(), lambda: remote().start())

    def sent(ship):
        is_self, local, remote = ship
        either(is_self, lambda: None, lambda: remote().wait_send())

    def cycle_body(cycle, carry):
        first = lax.rem(cycle * layers, 2)

        def load_body(t, carry2):
            @pl.when(cycle == 0)
            def _():
                for q in range(4):
                    for s in range(2):
                        await_bytes(ht.at[t, q, :, 32 * s:32 * s + 32, :], irecv.at[t, q, s])

            @pl.when(cycle > 0)
            def _():
                for s in range(4):
                    await_bytes(ht.at[t, s], grecv.at[t, s])
            for q in range(4):
                part = ht[t, q].reshape(4 * VARS, LANE).T
                hf[t, LANE * q:LANE * (q + 1), :] = part
                hb[first, t, 4 * c + q] = part.astype(BF16)
            share(first, t).start()

            @pl.when(cycle == 0)
            def _():
                for q in range(8):
                    a_copy(t, q).wait()
            await_share(first, t)
            lo = pl.multiple_of(CHUNK * t, CHUNK)
            state = hb[first, t].reshape(CHUNK, 4 * VARS)
            for tt in range(TILES):
                for r in range(2):
                    add = jnp.dot(a_rows(tt, r, lo, CHUNK), state, preferred_element_type=F32)
                    macc[tt, 256 * r:256 * (r + 1), :] = macc[tt, 256 * r:256 * (r + 1), :] + add
            return carry2

        macc[...] = jnp.zeros_like(macc)
        lax.fori_loop(0, TILES, load_body, 0)

        @pl.when(cycle == 0)
        def _():
            for t in range(TILES):
                for q in range(4):
                    for h in range(2):
                        sent(init_piece(h, t, q))

        def finish(layer, t):
            nxt = lax.rem(cycle * layers + layer + 1, 2)
            sums = [None, None]
            for n in range(8):
                for p in range(2):
                    lo = 256 * n
                    h = jnp.dot(mt[:, 128 * p:128 * (p + 1)], wp[layer, :, lo:lo + 256], preferred_element_type=F32)
                    z = h * (C1 + C2 * (h * h))
                    q_act = (h + h * jnp.tanh(z)).astype(BF16)
                    part = jnp.dot(q_act, up[layer, lo:lo + 256, :], preferred_element_type=F32)
                    sums[p] = part if sums[p] is None else sums[p] + part
            for p in range(2):
                hf[t, :, 128 * p:128 * (p + 1)] = hf[t, :, 128 * p:128 * (p + 1)] + sums[p]

            @pl.when(layer < layers - 1)
            def _():
                for q in range(4):
                    hb[nxt, t, 4 * c + q] = hf[t, LANE * q:LANE * (q + 1), :].astype(BF16)
                share(nxt, t).start()

            @pl.when(layer == layers - 1)
            def _():
                for q in range(4):
                    st[t, q] = hf[t, LANE * q:LANE * (q + 1), :].T.reshape(4, VARS, LANE)
                for q in range(4):
                    start(f_ship(t, q))

        def layer_body(layer, carry2):
            cur = lax.rem(cycle * layers + layer, 2)
            late = TILES - 1
            early_size = CHUNK * late

            def first_mix():
                def lates(r, core):
                    lo = pl.multiple_of(early_size + 512 * core, 512)
                    return jnp.dot(a_rows(0, r, lo, 512), hb[cur, late, pl.ds(4 * core, 4)].reshape(512, 4 * VARS), preferred_element_type=F32)
                early = []
                for r in range(2):
                    acc = jnp.dot(a_rows(0, r, 0, early_size), hb[cur, :late].reshape(early_size, 4 * VARS), preferred_element_type=F32)
                    early.append(acc + lates(r, c))
                await_share(cur, late)
                for r in range(2):
                    mt[256 * r:256 * (r + 1), :] = (early[r] + lates(r, 1 - c)).astype(BF16)

            def full_mix(t):
                state = hb[cur].reshape(COLS, 4 * VARS)
                for r in range(2):
                    mixed = jnp.dot(a_rows(t, r, 0, COLS), state, preferred_element_type=F32)
                    mt[256 * r:256 * (r + 1), :] = mixed.astype(BF16)

            def tile_body(t, carry3):
                full_mix(t)
                finish(layer, t)
                return carry3

            for t in range(late):
                await_share(cur, t)
            first_mix()
            finish(layer, 0)
            for t in range(TILES):
                share(cur, t).wait_send()
            return lax.fori_loop(1, TILES, tile_body, carry2)

        def first_layer(t, carry2):
            mt[...] = macc[t].astype(BF16)
            finish(cycle * 0, t)
            return carry2

        lax.fori_loop(0, TILES, first_layer, 0)
        for t in range(TILES):
            share(first, t).wait_send()
        lax.fori_loop(1, layers, layer_body, 0)

        @pl.when(cycle > 0)
        def _():
            for t in range(TILES):
                for n in range(4):
                    sent(g_ship(t, n))

        def analysis_body(t, carry2):
            for s in range(4):
                await_bytes(xin.at[t, 4 * s:4 * s + 4], frecv.at[t, s])

            def write(k, row, a, b):
                gst[t, k, row:row + 8, :] = a
                gst[t, k, row + 8:row + 16, :] = b
            analyse_tile(xin, t, idx_ref, obs_ref.at[cycle], prec_ref, rho_ref[0], ob, xa, mref, yo, gp, bm, zm, tm, wa, write)

            @pl.when(cycle < cycles - 1)
            def _():
                for n in range(4):
                    start(g_ship(t, n))

            @pl.when(cycle == cycles - 1)
            def _():
                for n in range(8):
                    start(o_ship(t, n))
            return carry2

        lax.fori_loop(0, TILES, analysis_body, 0)
        for t in range(TILES):
            for q in range(4):
                sent(f_ship(t, q))
        return carry

    lax.fori_loop(0, cycles, cycle_body, 0)
    for t in range(TILES):
        for n in range(8):
            sent(o_ship(t, n))
        for s in range(8):
            lo = BLK * s + LANE * t
            await_bytes(out_ref.at[:, :, lo:lo + LANE], orecv.at[t, s])


def run_cycles(ens_t, w_in, w_out_t, mix_op, obs_t, prec_t, obs_idx, rho):
    vm = pl.BlockSpec(memory_space=pltpu.VMEM)
    sm = pl.BlockSpec(memory_space=pltpu.SMEM)
    hbm = pl.BlockSpec(memory_space=pl.ANY)
    dma = pltpu.SemaphoreType.DMA
    layers, cycles = w_in.shape[0], obs_t.shape[0]
    return pl.pallas_call(
        functools.partial(cycle_kernel, layers, cycles),
        out_shape=jax.ShapeDtypeStruct((4, 32, COLS), F32),
        in_specs=[hbm, hbm, hbm, hbm, vm, vm, sm, sm],
        out_specs=hbm,
        scratch_shapes=[
            pltpu.VMEM((HALF, COLS), BF16),
            pltpu.VMEM((2, TILES, 8, LANE, 4 * VARS), BF16),
            pltpu.VMEM((TILES, ROWS, 4 * VARS), F32),
            pltpu.VMEM((ROWS, 4 * VARS), BF16),
            pltpu.VMEM((TILES, ROWS, 4 * VARS), F32),
            pltpu.VMEM((TILES, 4, 4, VARS, LANE), F32),
            pltpu.VMEM((TILES, 4, 4, VARS, LANE), F32),
            pltpu.VMEM((TILES, K, VARS, LANE), F32),
            pltpu.VMEM((TILES, K, VARS, LANE), F32),
            pltpu.VMEM((2, layers, VARS, HID // 2), BF16),
            pltpu.VMEM((2, layers, VARS, HID // 2), BF16),
            pltpu.VMEM((layers, 2 * VARS, 2 * HID), BF16),
            pltpu.VMEM((layers, 2 * HID, 2 * VARS), BF16),
            pltpu.VMEM((64, LANE), F32),
            pltpu.VMEM((K * VARS, LANE), F32),
            pltpu.VMEM((VARS, LANE), F32),
            pltpu.VMEM((512, LANE), F32),
            pltpu.VMEM((512, LANE), F32),
            pltpu.VMEM((2, 256, LANE), F32),
            pltpu.VMEM((2, 256, LANE), F32),
            pltpu.VMEM((256, LANE), F32),
            pltpu.VMEM((256, LANE), F32),
            dma((TILES, 8)),
            dma((2, TILES, 4)),
            dma((TILES, 4, 2)),
            dma((2,)),
            dma((2, 2)),
            dma((2, TILES)),
            dma((2, TILES)),
            dma((TILES, 4)),
            dma((TILES, 4)),
            dma((TILES, 4)),
            dma((TILES, 4)),
            dma((TILES, 8)),
            dma((TILES, 8)),
        ],
        compiler_params=pltpu.CompilerParams(collective_id=1, has_side_effects=True, vmem_limit_bytes=VMEM_LIMIT),
        name="cycle_all",
    )(ens_t, w_in, w_out_t, mix_op, obs_t, prec_t, obs_idx, rho)


def solution(mesh):
    def local_step(ens_local, mix_op, w_in, w_out, obs_val, obs_prec, obs_idx, inflation):
        out = run_cycles(
            jnp.transpose(ens_local, (0, 2, 1)), w_in, jnp.transpose(w_out, (0, 2, 1)), mix_op,
            jnp.transpose(obs_val, (0, 2, 1)), jnp.transpose(obs_prec, (1, 0)), obs_idx, inflation)
        return jnp.transpose(out, (0, 2, 1))

    member_spec = P(("case", "ens"), None, "model")
    col_axes = ("case", "ens", "model")
    in_specs = (member_spec, P(None, None), P(None, None, "model"), P(None, "model", None), P(None, col_axes, None), P(col_axes, None), P(None), P(None))
    return jax.shard_map(local_step, mesh=mesh, in_specs=in_specs, out_specs=member_spec, check_vma=False)
```
